32 devices in a mesh: aux: 4 (over z), orb: 8 (over y, x, core).
Axes of the slice: x: 2, y: 2, z: 4, core: 2. Of those that a mesh axis runs over, the one named last changes fastest.
Arguments:
- half: bfloat16 [64, 384, 3072], P('aux', 'orb'), may hold values from -1.25 to 1.25
- metric: bfloat16 [64, 64], P('aux'), may hold values from -1 to 2
- survive: int32 [4, 16, 24], P('aux', 'orb'), may hold values 0 or 1
Outputs:
- exchange_k: float32 [3072, 3072], P('orb', 'aux')
The draws below stay inside these ranges and needn't reach their ends.
All inputs are finite; a program needn't handle non-finite values. No bound on the sum of `survive` on one device may be relied on, other than what follows from the above.
Results may differ from the reference program's by a relative error of at most 0.00098.
Values may be sent and summed in bfloat16 or wider, within the bound.
A program may use at most 128 MiB of HBM per device.

```python
import jax
import jax.numpy as jnp
from jax import lax

NOCC = 384
OCCB = 24
NAO = 3072
AOBLK = 128
NAUX = 64
N_AUX = 4


def draw_metric(key, part):
    first_key = jax.random.fold_in(key, 11)
    second_key = jax.random.fold_in(key, 12)
    spread = jax.random.normal(first_key, (NAUX, NAUX), jnp.float32) * (0.6 / NAUX ** 0.5)
    diagonal_part = jax.random.uniform(second_key, (NAUX,), jnp.float32, 0.9, 1.1)
    return (spread + jnp.diag(diagonal_part)).astype(jnp.bfloat16)


def set_ends(entries, own_key, low, largest):
    shape = entries.shape
    place = [jax.random.randint(jax.random.fold_in(own_key, axis), (), 0, shape[axis]) for axis in range(len(shape))]
    entries = entries.at[tuple(place)].set(low)
    longest = shape.index(max(shape))
    place[longest] = (place[longest] + 1) % shape[longest]
    return entries.at[tuple(place)].set(largest)


def steps_of(key, shape, cuts, low, largest):
    def one(axis_at, shards_of):
        draws = jax.random.uniform(jax.random.fold_in(jax.random.fold_in(key, 6), axis_at), (shards_of,), jnp.float32, low / len(cuts), largest / len(cuts))
        return jnp.repeat(jnp.exp(draws), shape[axis_at] // shards_of).reshape((-1,) + (1,) * (len(shape) - axis_at - 1))

    level = one(*cuts[0])
    for cut in cuts[1:]:
        level = level * one(*cut)
    return level


def bell_draw(key, shape, scale, most, shards=(), kind=jnp.bfloat16):
    factor_of = steps_of(key, shape, shards, -0.22, 0.18) if shards else 1.0
    values = jax.random.normal(key, shape, jnp.float32) * scale * factor_of
    return jnp.minimum(jnp.maximum(values, -most), most).astype(kind)


def setup_inputs(seed: int = 0) -> dict:
    key_of = jax.random.split(jax.random.key(seed), 4)
    half = bell_draw(key_of[0], (NAUX, NOCC, NAO), ((NAUX * NOCC) ** -0.25), 1.25, ((0, 4), (1, 8)))
    metric = draw_metric(jax.random.fold_in(key_of[3], 71), 0)
    survive = set_ends((jax.random.randint(key_of[2], (N_AUX, NOCC // OCCB, NAO // AOBLK), 0, 3) < 2).astype(jnp.int32), jax.random.fold_in(key_of[2], 1), 0, 1)
    return dict(half=half, metric=metric, survive=survive)


def reference(half, metric, survive):
    blocks_aux, blocks_occ, blocks_ao = survive.shape
    aux_count, occ_count, ao_count = half.shape
    gate = survive.astype(jnp.bfloat16)
    shaped = half.reshape(blocks_aux, aux_count // blocks_aux, blocks_occ, occ_count // blocks_occ, blocks_ao, ao_count // blocks_ao)
    masked = (shaped * gate[:, None, :, None, :, None]).reshape(aux_count, occ_count, ao_count)
    occ_width = occ_count // blocks_occ

    def accumulate(totals, block_index):
        occ_rows = lax.dynamic_slice_in_dim(masked, block_index * occ_width, occ_width, 1)
        fitted = jnp.dot(metric, occ_rows.reshape(aux_count, -1), preferred_element_type=jnp.float32)
        fitted = fitted.astype(jnp.bfloat16).reshape(-1, ao_count)
        update = lax.dot_general(fitted, fitted, (((0,), (0,)), ((), ())), preferred_element_type=jnp.float32)
        return totals + update, None

    exchange_k, _ = lax.scan(accumulate, jnp.zeros((ao_count, ao_count), jnp.float32), jnp.arange(blocks_occ, dtype=jnp.int32))
    return exchange_k
```

```python
import functools

import jax
import jax.numpy as jnp
from jax import lax
from jax.experimental import pallas as pl
from jax.experimental.pallas import tpu as pltpu
from jax.sharding import PartitionSpec as P

MESH = pl.DeviceIdType.MESH
F32 = jnp.float32


def gated(half, survive):
    aux_local, occ_local, ao_count = half.shape
    blocks_aux, blocks_occ, blocks_ao = survive.shape
    gate = survive.astype(jnp.bfloat16)
    shaped = half.reshape(
        blocks_aux, aux_local, blocks_occ, occ_local // blocks_occ, blocks_ao, ao_count // blocks_ao
    )
    return (shaped * gate[:, None, :, None, :, None]).reshape(aux_local, occ_local, ao_count)


def plain(half, metric, survive):
    aux_local, occ_local, ao_count = half.shape
    portion = lax.all_gather(gated(half, survive), "aux", axis=0, tiled=True)
    fit_total = jnp.dot(metric, portion.reshape(portion.shape[0], -1), preferred_element_type=F32)
    fitted = fit_total.astype(jnp.bfloat16).reshape(aux_local, occ_local, ao_count)
    group_width = ao_count // lax.axis_size("orb")
    row_start = lax.axis_index("orb") * group_width
    flat_rows = lax.all_gather(fitted, "orb", axis=1, tiled=True).reshape(-1, ao_count)
    left_rows = lax.dynamic_slice_in_dim(flat_rows, row_start, group_width, 1)
    partial_k = lax.dot_general(
        left_rows, flat_rows, (((0,), (0,)), ((), ())), preferred_element_type=F32
    )
    return lax.psum_scatter(partial_k, "aux", scatter_dimension=1, tiled=True)

TOP = 32000.0
FINE = 256.0


def kernel(
    aux_local, m_ref, metric_ref, out_ref, held, fit, left, acc, whole, kron_ref,
    rs_out, rs_in, z_out, z_in, swap_out, swap_in,
    gs, gr, zs, zr, fs, fr, rs, rr, cs, cr, ws, wr,
):
    z = lax.axis_index("aux")
    orb = lax.axis_index("orb")
    n_aux = m_ref.shape[0]
    parts = held.shape[1]
    unit = m_ref.shape[1] // parts
    panel = acc.shape[1]
    width = acc.shape[2]
    piece = width // n_aux
    chip = orb // 2
    core = orb % 2
    x_chip = chip + 1 - 2 * (chip % 2)
    y_chip = chip + 2 - 4 * (chip // 2)
    partner = orb + 1 - 2 * core
    other_chip = core * x_chip + (1 - core) * y_chip
    rs_peer = 2 * other_chip + core
    side = z // 2
    mate = z + 1 - 2 * (z % 2)
    far_inner = 2 - side
    far_end = 3 - 3 * side
    inner = (z + 1) // 2 % 2 == 1

    barrier = pltpu.get_barrier_semaphore()
    for d in (1, 2, 3):
        pl.semaphore_signal(
            barrier, inc=1, device_id={"aux": (z + d) % n_aux, "orb": orb}, device_id_type=MESH
        )
    near = (partner, 2 * x_chip, 2 * x_chip + 1, 2 * y_chip, 2 * y_chip + 1)
    for o in near:
        pl.semaphore_signal(barrier, inc=1, device_id={"aux": z, "orb": o}, device_id_type=MESH)
    pl.semaphore_wait(barrier, 8)

    def remote(src, dst, send, recv, a, o):
        return pltpu.make_async_remote_copy(
            src_ref=src, dst_ref=dst, send_sem=send, recv_sem=recv,
            device_id={"aux": a, "orb": o}, device_id_type=MESH,
        )

    def span(s):
        return pl.ds(pl.multiple_of(s * unit, unit), unit)

    first = 1 + z % 2
    third = 3 - 3 * side
    second = 6 - first - third - z
    spread = []
    for s, there in enumerate((first, second, third)):
        for q in range(parts):
            copy = remote(
                m_ref.at[there, pl.ds(q * unit, unit)], held.at[0, q, span(z)],
                zs.at[s * parts + q], zr.at[z * parts + q], there, orb,
            )
            copy.start()
            spread.append(copy)

    shared = []

    def share(source, r, q, block):
        n = r * parts + q
        targets = ((1, partner), (2 + core, 2 * x_chip), (2 + core, 2 * y_chip + 1))
        for k, (slot, o) in enumerate(targets):
            copy = remote(
                block, held.at[slot, q, span(source)], fs.at[k * 4 * parts + n],
                fr.at[slot * 4 * parts + n], z, o,
            )
            copy.start()
            shared.append(copy)

    sources = (z, mate, far_inner, far_end)

    def arrive(r, q):
        source = sources[r]
        here = held.at[0, q, span(source)]
        remote(here, here, zs.at[q], zr.at[source * parts + q], mate, orb).wait_recv()
        share(source, r, q, here)

    for q in range(parts):
        share(z, 0, q, m_ref.at[z, pl.ds(q * unit, unit)])
    metric_rows = pl.ds(pl.multiple_of(z * aux_local, aux_local), aux_local)
    gather = []
    for d in (1, 3, 2):
        copy = remote(metric_ref, whole.at[metric_rows], gs.at[d], gr.at[d], (z + d) % n_aux, orb)
        copy.start()
        gather.append(copy)

    def build_kron():
        whole[metric_rows, :] = metric_ref[...]
        for copy in gather:
            copy.wait_recv()
        depth, wide = kron_ref.shape[0], whole.shape[1]

        def aux_of(r):
            return lax.div(r, unit) * aux_local + lax.rem(r, aux_local)

        def orbital_of(r):
            return lax.div(lax.rem(r, unit), aux_local)

        i32, bf16 = jnp.int32, kron_ref.dtype
        by_row = aux_of(lax.broadcasted_iota(i32, (wide, depth), 1))
        pick = jnp.where(by_row == lax.broadcasted_iota(i32, (wide, depth), 0), 1.0, 0.0)
        spread_cols = jnp.dot(whole[...], pick.astype(bf16), preferred_element_type=F32).astype(bf16)
        by_col = aux_of(lax.broadcasted_iota(i32, (depth, whole.shape[0]), 0))
        take = jnp.where(by_col == lax.broadcasted_iota(i32, (depth, whole.shape[0]), 1), 1.0, 0.0)
        both = jnp.dot(take.astype(bf16), spread_cols, preferred_element_type=F32)
        same = orbital_of(lax.broadcasted_iota(i32, (depth, depth), 0)) == orbital_of(
            lax.broadcasted_iota(i32, (depth, depth), 1)
        )
        kron_ref[...] = jnp.where(same, both, 0.0).astype(bf16)

    slab = kron_ref.shape[0]

    def aligned(start, size, unit_of=128):
        return pl.ds(pl.multiple_of(start, unit_of), size)

    def fit_part(q):
        @pl.loop(0, 4)
        def _(slot):
            rows = aligned(slot * slab, slab)

            def put(at, columns):
                fit[rows, at] = jnp.dot(
                    kron_ref[...], held[slot, q, :, columns], preferred_element_type=F32
                ).astype(fit.dtype)

            for b in range(n_aux):
                put(pl.ds(b * piece, piece), aligned((2 * b + core) * piece, piece))
            put(pl.ds(width, panel), aligned(chip * panel, panel))
            put(pl.ds(width + panel, panel), aligned(other_chip * panel, panel))

        left[0] = fit[:, width : width + panel].T
        left[1] = fit[:, width + panel :].T

    def contract(p, start, size, begin):
        at = aligned(start, size)
        more = jnp.dot(left[p], fit[:, at], preferred_element_type=F32)
        acc[p, :, at] = more if begin else acc[p, :, at] + more

    def contract_all(begin):
        step = 512

        @pl.loop(0, width // step)
        def _(t):
            contract(0, t * step, step, begin)
            contract(1, t * step, step, begin)

    strip = 64

    def block_at(b):
        return aligned(b * piece, piece)

    def quantize(p, b, target):
        at = block_at(b)

        def tops(t, top):
            rows = acc[p, aligned(t * strip, strip, strip), at]
            return jnp.maximum(top, jnp.max(jnp.abs(rows).reshape(strip // 8, 8, piece), axis=0))

        top = lax.fori_loop(0, panel // strip, tops, jnp.zeros((8, piece), F32))
        top = jnp.maximum(jnp.max(top, axis=0, keepdims=True), 1e-30)
        level = jnp.ceil(jnp.log2(top) * FINE)
        scale = TOP * jnp.exp2(level * (-1.0 / FINE))

        @pl.loop(0, panel // strip)
        def _(t):
            rows = aligned(t * strip, strip, strip)
            target[rows, :] = jnp.round(acc[p, rows, at] * scale).astype(jnp.int32).astype(jnp.int16)

        target[pl.ds(panel, 16), :] = jnp.broadcast_to(
            level.astype(jnp.int32), (16, piece)
        ).astype(jnp.int16)

    def add_in(source, b):
        at = block_at(b)
        level = source[pl.ds(panel, 16), :].astype(F32)[:1]
        scale = jnp.exp2(level * (1.0 / FINE)) * (1.0 / TOP)

        @pl.loop(0, panel // strip)
        def _(t):
            rows = aligned(t * strip, strip, strip)
            acc[0, rows, at] = acc[0, rows, at] + source[rows, :].astype(F32) * scale

    def slots_of(q):
        for slot in (1, 2, 3):
            for r in range(4):
                here = held.at[slot, q, span(sources[r])]
                remote(
                    here, here, fs.at[0], fr.at[slot * 4 * parts + r * parts + q], z, partner
                ).wait_recv()

    held_own = [(q, q * unit) for q in range(parts)]
    for q, at in held_own:
        held[0, q, span(z), :] = m_ref[z, pl.ds(at, unit), :]
    build_kron()
    for r in (1, 2):
        for q in range(parts):
            arrive(r, q)
    arrive(3, 0)
    arrive(3, 1)
    slots_of(0)
    fit_part(0)
    contract_all(True)
    arrive(3, 2)
    slots_of(1)
    fit_part(1)
    contract_all(False)
    slots_of(2)
    fit_part(2)

    order = (far_inner, far_end, mate, z)
    far_half, near_half = (1 - side) * 2 * piece, side * 2 * piece
    reduce_copies = []

    def give(n):
        quantize(1, order[n], rs_out.at[n])
        copy = remote(rs_out.at[n], rs_in.at[n], rs.at[n], rr.at[n], z, rs_peer)
        copy.start()
        reduce_copies.append(copy)

    contract(1, far_half, 2 * piece, False)
    give(0)
    give(1)
    contract(1, near_half, 2 * piece, False)
    give(2)
    give(3)
    contract(0, far_half, 2 * piece, False)
    contract(0, near_half, 2 * piece, False)

    def along(n, there, into):
        return remote(z_out.at[n], z_in.at[into], cs.at[n], cr.at[into], there, orb)

    up_to_mate = (along(0, mate, 0), along(1, mate, 1))
    to_mate = along(2, mate, 2)
    across = (along(0, far_inner, 3), along(1, far_end, 3))
    for n in (0, 1):
        reduce_copies[n].wait_recv()
        add_in(rs_in.at[n], order[n])

        @pl.when(jnp.logical_not(inner))
        def _():
            quantize(0, order[n], z_out.at[n])
            up_to_mate[n].start()

    reduce_copies[2].wait_recv()
    add_in(rs_in.at[2], mate)
    quantize(0, mate, z_out.at[2])
    to_mate.start()
    reduce_copies[3].wait_recv()
    add_in(rs_in.at[3], z)

    @pl.when(inner)
    def _():
        for n in (0, 1):
            up_to_mate[n].wait_recv()
            add_in(z_in.at[n], order[n])
            quantize(0, order[n], z_out.at[n])
            across[n].start()

    to_mate.wait_recv()
    add_in(z_in.at[2], z)
    across[0].wait_recv()
    add_in(z_in.at[3], z)
    rows = out_ref.shape[0]
    own_at = block_at(z)
    swap_out[...] = acc[0, aligned((1 - core) * rows, rows), own_at]
    swap = remote(swap_out, swap_in, ws.at[0], wr.at[0], z, partner)
    swap.start()
    out_ref[:, aligned(core * piece, piece)] = acc[0, aligned(core * rows, rows), own_at]
    swap.wait_recv()
    out_ref[:, aligned((1 - core) * piece, piece)] = swap_in[...]

    @pl.when(inner)
    def _():
        for copy in across:
            copy.wait_send()

    @pl.when(jnp.logical_not(inner))
    def _():
        for copy in up_to_mate:
            copy.wait_send()

    for copy in (*gather, *spread, *shared, *reduce_copies, to_mate, swap):
        copy.wait_send()


def direct(half, metric, survive):
    aux_local, occ_local, ao = half.shape
    n_aux, n_orb = lax.axis_size("aux"), lax.axis_size("orb")
    part = occ_local // n_aux
    blocks = gated(half, survive).transpose(1, 0, 2).reshape(n_aux, part * aux_local, ao)
    n_fit = n_aux * aux_local
    width = -(-n_fit // 128) * 128
    metric = jnp.pad(metric, ((0, 0), (0, width - n_fit)))
    parts = 3
    slab = n_fit * part // parts
    rows, cols = ao // n_orb, ao // n_aux
    panel, half_width = 2 * rows, ao // 2
    piece = half_width // n_aux
    dma = pltpu.SemaphoreType.DMA
    bf16, i16 = jnp.bfloat16, jnp.int16
    return pl.pallas_call(
        functools.partial(kernel, aux_local),
        out_shape=jax.ShapeDtypeStruct((rows, cols), F32),
        in_specs=[pl.BlockSpec(memory_space=pltpu.VMEM)] * 2,
        out_specs=pl.BlockSpec(memory_space=pltpu.VMEM),
        scratch_shapes=[
            pltpu.VMEM((4, parts, slab, ao), bf16),
            pltpu.VMEM((4 * slab, half_width + 2 * panel), bf16),
            pltpu.VMEM((2, panel, 4 * slab), bf16),
            pltpu.VMEM((2, panel, half_width), F32),
            pltpu.VMEM((n_fit, width), bf16),
            pltpu.VMEM((slab, slab), bf16),
            pltpu.VMEM((4, panel + 16, piece), i16),
            pltpu.VMEM((4, panel + 16, piece), i16),
            pltpu.VMEM((3, panel + 16, piece), i16),
            pltpu.VMEM((4, panel + 16, piece), i16),
            pltpu.VMEM((rows, piece), F32),
            pltpu.VMEM((rows, piece), F32),
            dma((4,)), dma((4,)),
            dma((3 * parts,)), dma((n_aux * parts,)),
            dma((12 * parts,)), dma((16 * parts,)),
            dma((4,)), dma((4,)),
            dma((3,)), dma((4,)),
            dma((1,)), dma((1,)),
        ],
        compiler_params=pltpu.CompilerParams(
            collective_id=0, has_side_effects=True, vmem_limit_bytes=66 * 1000 * 1000
        ),
    )(blocks, metric)


def solution(mesh):
    square = mesh.shape["aux"] == 4 and mesh.shape["orb"] == 8
    return jax.shard_map(
        direct if square else plain,
        mesh=mesh,
        in_specs=(P("aux", "orb", None), P("aux", None), P("aux", "orb", None)),
        out_specs=P("orb", "aux"),
        check_vma=False,
    )
```

```python
import functools

import jax
import jax.numpy as jnp
from jax import lax
from jax.experimental import pallas as pl
from jax.experimental.pallas import tpu as pltpu
from jax.sharding import PartitionSpec as P

MESH = pl.DeviceIdType.MESH
F32 = jnp.float32


def gated(half, survive):
    aux_local, occ_local, ao_count = half.shape
    blocks_aux, blocks_occ, blocks_ao = survive.shape
    gate = survive.astype(jnp.bfloat16)
    shaped = half.reshape(
        blocks_aux, aux_local, blocks_occ, occ_local // blocks_occ, blocks_ao, ao_count // blocks_ao
    )
    return (shaped * gate[:, None, :, None, :, None]).reshape(aux_local, occ_local, ao_count)


def plain(half, metric, survive):
    aux_local, occ_local, ao_count = half.shape
    portion = lax.all_gather(gated(half, survive), "aux", axis=0, tiled=True)
    fit_total = jnp.dot(metric, portion.reshape(portion.shape[0], -1), preferred_element_type=F32)
    fitted = fit_total.astype(jnp.bfloat16).reshape(aux_local, occ_local, ao_count)
    group_width = ao_count // lax.axis_size("orb")
    row_start = lax.axis_index("orb") * group_width
    flat_rows = lax.all_gather(fitted, "orb", axis=1, tiled=True).reshape(-1, ao_count)
    left_rows = lax.dynamic_slice_in_dim(flat_rows, row_start, group_width, 1)
    partial_k = lax.dot_general(
        left_rows, flat_rows, (((0,), (0,)), ((), ())), preferred_element_type=F32
    )
    return lax.psum_scatter(partial_k, "aux", scatter_dimension=1, tiled=True)

TOP = 32000.0
FINE = 256.0


def kernel(
    aux_local, m_ref, metric_ref, out_ref, held, fit, left, acc, whole, kron_ref,
    rs_out, rs_in, z_out, z_in,
    gs, gr, zs, zr, fs, fr, rs, rr, cs, cr, ws, wr,
):
    z = lax.axis_index("aux")
    orb = lax.axis_index("orb")
    n_aux = m_ref.shape[0]
    parts = held.shape[1]
    unit = m_ref.shape[1] // parts
    panel = acc.shape[1]
    rows = panel // 2
    slab = kron_ref.shape[0]
    chip = orb // 2
    core = orb % 2
    x, y = chip % 2, chip // 2
    x_chip = chip + 1 - 2 * x
    y_chip = chip + 2 - 4 * y
    partner = orb + 1 - 2 * core
    other_chip = core * x_chip + (1 - core) * y_chip
    rs_peer = 2 * other_chip + core
    unused = core * (3 - 3 * y) + (1 - core) * (1 + x)
    third = 6 - unused - chip - other_chip
    side = z // 2
    end = z % 3 == 0
    mate = z + 1 - 2 * (z % 2)
    near_block = core * (1 + side) + (1 - core) * 3 * side
    far_block = 3 - near_block
    holder = near_block == z

    barrier = pltpu.get_barrier_semaphore()
    for d in (1, 2, 3):
        pl.semaphore_signal(
            barrier, inc=1, device_id={"aux": (z + d) % n_aux, "orb": orb}, device_id_type=MESH
        )
    for o in (partner, 2 * x_chip, 2 * x_chip + 1, 2 * y_chip, 2 * y_chip + 1):
        pl.semaphore_signal(barrier, inc=1, device_id={"aux": z, "orb": o}, device_id_type=MESH)
    pl.semaphore_wait(barrier, 8)

    def remote(src, dst, send, recv, a, o):
        return pltpu.make_async_remote_copy(
            src_ref=src, dst_ref=dst, send_sem=send, recv_sem=recv,
            device_id={"aux": a, "orb": o}, device_id_type=MESH,
        )

    def aligned(start, size, unit_of=128):
        return pl.ds(pl.multiple_of(start, unit_of), size)

    def span(s):
        return aligned(s * unit, unit, unit)

    metric_rows = aligned(z * aux_local, aux_local, aux_local)
    gather = []
    for d in (1, 3, 2):
        copy = remote(metric_ref, whole.at[metric_rows], gs.at[d], gr.at[d], (z + d) % n_aux, orb)
        copy.start()
        gather.append(copy)

    spread = []
    there_last = 2 - z - z % 2 + 3 * side
    for s, there in enumerate((3 - 3 * side, 1 + z % 2, there_last)):
        for q in range(parts):
            copy = remote(
                m_ref.at[there, pl.ds(q * unit, unit)], held.at[0, q, span(z)],
                zs.at[s * parts + q], zr.at[z * parts + q], there, orb,
            )
            copy.start()
            spread.append(copy)

    sources = (z, 3 - 3 * (z % 2), (z + 2) % n_aux, 1 + z % 2)
    shared = []

    def recv_at(slot, r, q, k):
        return fr.at[((slot * 4 + r) * parts + q) * 2 + k]

    def share(r, q, whole_block, cut):
        source = sources[r]
        jobs = [(whole_block, partner, 1, pl.ds(0, 4 * panel), 0)]
        for o, slot, first, pair in (
            (2 * x_chip, 2 + core, 3 - 3 * x, 2 * x),
            (2 * y_chip + 1, 2 + core, 1 - y, 2 - y),
        ):
            one, two = aligned(first * panel, panel), aligned(pair * panel, 2 * panel)
            jobs += [(cut(one), o, slot, one, 0), (cut(two), o, slot, two, 1)]
        for n, (block, o, slot, columns, k) in enumerate(jobs):
            copy = remote(
                block, held.at[slot, q, span(source), columns],
                fs.at[(n * 4 + r) * parts + q], recv_at(slot, r, q, k), z, o,
            )
            copy.start()
            shared.append(copy)

    def arrive(r, q):
        at = span(sources[r])
        here = held.at[0, q, at]
        remote(here, here, zs.at[q], zr.at[sources[r] * parts + q], mate, orb).wait_recv()
        share(r, q, here, lambda columns: held.at[0, q, at, columns])

    def share_own(q):
        at = pl.ds(q * unit, unit)
        share(0, q, m_ref.at[z, at], lambda columns: m_ref.at[z, at, columns])

    for q in range(parts):
        share_own(q)

    def build_kron():
        whole[metric_rows, :] = metric_ref[...]
        for copy in gather:
            copy.wait_recv()
        depth, wide = kron_ref.shape[0], whole.shape[1]

        def aux_of(r):
            return lax.div(r, unit) * aux_local + lax.rem(r, aux_local)

        def orbital_of(r):
            return lax.div(lax.rem(r, unit), aux_local)

        i32, bf16 = jnp.int32, kron_ref.dtype
        by_row = aux_of(lax.broadcasted_iota(i32, (wide, depth), 1))
        pick = jnp.where(by_row == lax.broadcasted_iota(i32, (wide, depth), 0), 1.0, 0.0)
        spread_cols = jnp.dot(whole[...], pick.astype(bf16), preferred_element_type=F32).astype(bf16)
        by_col = aux_of(lax.broadcasted_iota(i32, (depth, whole.shape[0]), 0))
        take = jnp.where(by_col == lax.broadcasted_iota(i32, (depth, whole.shape[0]), 1), 1.0, 0.0)
        both = jnp.dot(take.astype(bf16), spread_cols, preferred_element_type=F32)
        same = orbital_of(lax.broadcasted_iota(i32, (depth, depth), 0)) == orbital_of(
            lax.broadcasted_iota(i32, (depth, depth), 1)
        )
        kron_ref[...] = jnp.where(same, both, 0.0).astype(bf16)

    def slots_of(q):
        first = core * y + (1 - core) * 3 * x
        pair = core * (1 + y) + (1 - core) * 2 * (1 - x)
        one, two = aligned(first * panel, panel), aligned(pair * panel, 2 * panel)
        for r in range(4):
            at = span(sources[r])
            for slot, k, columns in (
                (1, 0, pl.ds(0, 4 * panel)), (2, 0, one), (2, 1, two), (3, 0, one), (3, 1, two)
            ):
                here = held.at[slot, q, at, columns]
                remote(here, here, fs.at[0], recv_at(slot, r, q, k), z, partner).wait_recv()

    def fit_part(q):
        @pl.loop(0, 4)
        def _(slot):
            for n, p in enumerate((chip, other_chip, third)):
                fit[aligned(slot * slab, slab, slab), pl.ds(n * panel, panel)] = jnp.dot(
                    kron_ref[...], held[slot, q, :, aligned(p * panel, panel)],
                    preferred_element_type=F32,
                ).astype(fit.dtype)

        for n in range(2):
            left[n] = fit[:, n * panel : (n + 1) * panel].T

    def place(block):
        return jnp.where(block == chip, 0, jnp.where(block == other_chip, 1, 2))

    near, far = (near_block, side), (far_block, 1 - side)

    def block_at(block):
        return aligned(block[1] * panel, panel)

    def contract(p, block, begin):
        columns = fit[:, aligned(place(block[0]) * panel, panel)]
        at = block_at(block)
        more = jnp.dot(left[p], columns, preferred_element_type=F32)
        acc[p, :, at] = more if begin else acc[p, :, at] + more

    def contract_all(begin):
        for p in range(2):
            contract(p, far, begin)
            contract(p, near, begin)

    strip = 32
    halves = (1 - core, core)

    def quantize(p, block, h, target):
        at = block_at(block)

        def tops(t, top):
            some = acc[p, aligned(h * rows + t * strip, strip, strip), at]
            return jnp.maximum(top, jnp.max(jnp.abs(some).reshape(strip // 8, 8, panel), axis=0))

        top = lax.fori_loop(0, rows // strip, tops, jnp.zeros((8, panel), F32))
        top = jnp.maximum(jnp.max(top, axis=0, keepdims=True), 1e-30)
        level = jnp.ceil(jnp.log2(top) * FINE)
        scale = TOP * jnp.exp2(level * (-1.0 / FINE))

        @pl.loop(0, rows // strip)
        def _(t):
            some = acc[p, aligned(h * rows + t * strip, strip, strip), at]
            target[aligned(t * strip, strip, strip), :] = (
                jnp.round(some * scale).astype(jnp.int32).astype(jnp.int16)
            )

        target[pl.ds(rows, 16), :] = jnp.broadcast_to(
            level.astype(jnp.int32), (16, panel)
        ).astype(jnp.int16)

    def add_in(source, block, h):
        at = block_at(block)
        level = source[pl.ds(rows, 16), :].astype(F32)[:1]
        scale = jnp.exp2(level * (1.0 / FINE)) * (1.0 / TOP)

        @pl.loop(0, rows // strip)
        def _(t):
            here = aligned(h * rows + t * strip, strip, strip)
            some = source[aligned(t * strip, strip, strip), :].astype(F32)
            acc[0, here, at] = acc[0, here, at] + some * scale

    for q in range(parts):
        held[0, q, span(z), :] = m_ref[z, pl.ds(q * unit, unit), :]
    build_kron()
    for r in (1, 2):
        for q in range(parts):
            arrive(r, q)
    arrive(3, 0)
    arrive(3, 1)
    slots_of(0)
    fit_part(0)
    contract_all(True)
    arrive(3, 2)
    slots_of(1)
    fit_part(1)
    contract_all(False)
    slots_of(2)
    fit_part(2)

    given = []

    def give(block, n):
        for i, h in enumerate(halves):
            slot = 2 * n + i
            quantize(1, block, h, rs_out.at[slot])
            copy = remote(rs_out.at[slot], rs_in.at[slot], rs.at[slot], rr.at[slot], z, rs_peer)
            copy.start()
            given.append(copy)

    contract(1, far, False)
    give(far, 0)
    contract(1, near, False)
    give(near, 1)
    contract(0, far, False)
    contract(0, near, False)

    def along(n, into, there):
        return remote(z_out.at[n], z_in.at[into], cs.at[n], cr.at[into], there, orb)

    inward = [along(i, i, mate) for i in range(2)]
    to_mate = [along(2 + i, 2 + i, mate) for i in range(2)]
    across = [along(i, 4 + i, far_block) for i in range(2)]
    for i, h in enumerate(halves):
        given[i].wait_recv()
        add_in(rs_in.at[i], far, h)

        @pl.when(end)
        def _():
            quantize(0, far, h, z_out.at[i])
            inward[i].start()

    for i, h in enumerate(halves):
        given[2 + i].wait_recv()
        add_in(rs_in.at[2 + i], near, h)

        @pl.when(jnp.logical_not(holder))
        def _():
            quantize(0, near, h, z_out.at[2 + i])
            to_mate[i].start()

    @pl.when(jnp.logical_not(end))
    def _():
        for i, h in enumerate(halves):
            inward[i].wait_recv()
            add_in(z_in.at[i], far, h)
            quantize(0, far, h, z_out.at[i])
            across[i].start()

    own_at = block_at(near)
    last = remote(
        acc.at[0, aligned((1 - core) * rows, rows, rows), own_at], out_ref,
        ws.at[0], wr.at[0], z, partner,
    )

    @pl.when(holder)
    def _():
        for i, h in enumerate(halves):
            to_mate[i].wait_recv()
            add_in(z_in.at[2 + i], near, h)
        for i, h in enumerate(halves):
            across[i].wait_recv()
            add_in(z_in.at[4 + i], near, h)
            if i == 0:
                last.start()
        out_ref[...] = acc[0, aligned(core * rows, rows, rows), own_at]
        last.wait_send()

    @pl.when(jnp.logical_not(holder))
    def _():
        last.wait_recv()
        for copy in to_mate:
            copy.wait_send()

    @pl.when(end)
    def _():
        for copy in inward:
            copy.wait_send()

    @pl.when(jnp.logical_not(end))
    def _():
        for copy in across:
            copy.wait_send()

    for copy in (*gather, *spread, *shared, *given):
        copy.wait_send()


def direct(half, metric, survive):
    aux_local, occ_local, ao = half.shape
    n_aux, n_orb = lax.axis_size("aux"), lax.axis_size("orb")
    part = occ_local // n_aux
    blocks = gated(half, survive).transpose(1, 0, 2).reshape(n_aux, part * aux_local, ao)
    n_fit = n_aux * aux_local
    width = -(-n_fit // 128) * 128
    metric = jnp.pad(metric, ((0, 0), (0, width - n_fit)))
    parts = 3
    slab = n_fit * part // parts
    rows, panel = ao // n_orb, ao // n_aux
    dma = pltpu.SemaphoreType.DMA
    bf16, i16 = jnp.bfloat16, jnp.int16
    return pl.pallas_call(
        functools.partial(kernel, aux_local),
        out_shape=jax.ShapeDtypeStruct((rows, panel), F32),
        in_specs=[pl.BlockSpec(memory_space=pltpu.VMEM)] * 2,
        out_specs=pl.BlockSpec(memory_space=pltpu.VMEM),
        scratch_shapes=[
            pltpu.VMEM((4, parts, slab, ao), bf16),
            pltpu.VMEM((4 * slab, 3 * panel), bf16),
            pltpu.VMEM((2, panel, 4 * slab), bf16),
            pltpu.VMEM((2, panel, 2 * panel), F32),
            pltpu.VMEM((n_fit, width), bf16),
            pltpu.VMEM((slab, slab), bf16),
            pltpu.VMEM((4, rows + 16, panel), i16),
            pltpu.VMEM((4, rows + 16, panel), i16),
            pltpu.VMEM((4, rows + 16, panel), i16),
            pltpu.VMEM((6, rows + 16, panel), i16),
            dma((4,)), dma((4,)),
            dma((3 * parts,)), dma((n_aux * parts,)),
            dma((20 * parts,)), dma((32 * parts,)),
            dma((4,)), dma((4,)),
            dma((4,)), dma((6,)),
            dma((1,)), dma((1,)),
        ],
        compiler_params=pltpu.CompilerParams(
            collective_id=0, has_side_effects=True, vmem_limit_bytes=66 * 1000 * 1000
        ),
    )(blocks, metric)


def solution(mesh):
    square = mesh.shape["aux"] == 4 and mesh.shape["orb"] == 8
    return jax.shard_map(
        direct if square else plain,
        mesh=mesh,
        in_specs=(P("aux", "orb", None), P("aux", None), P("aux", "orb", None)),
        out_specs=P("orb", "aux"),
        check_vma=False,
    )
```

```python
import functools

import jax
import jax.numpy as jnp
from jax import lax
from jax.experimental import pallas as pl
from jax.experimental.pallas import tpu as pltpu
from jax.sharding import PartitionSpec as P

MESH = pl.DeviceIdType.MESH
F32 = jnp.float32


def gated(half, survive):
    aux_local, occ_local, ao_count = half.shape
    blocks_aux, blocks_occ, blocks_ao = survive.shape
    gate = survive.astype(jnp.bfloat16)
    shaped = half.reshape(
        blocks_aux, aux_local, blocks_occ, occ_local // blocks_occ, blocks_ao, ao_count // blocks_ao
    )
    return (shaped * gate[:, None, :, None, :, None]).reshape(aux_local, occ_local, ao_count)


def plain(half, metric, survive):
    aux_local, occ_local, ao_count = half.shape
    portion = lax.all_gather(gated(half, survive), "aux", axis=0, tiled=True)
    fit_total = jnp.dot(metric, portion.reshape(portion.shape[0], -1), preferred_element_type=F32)
    fitted = fit_total.astype(jnp.bfloat16).reshape(aux_local, occ_local, ao_count)
    group_width = ao_count // lax.axis_size("orb")
    row_start = lax.axis_index("orb") * group_width
    flat_rows = lax.all_gather(fitted, "orb", axis=1, tiled=True).reshape(-1, ao_count)
    left_rows = lax.dynamic_slice_in_dim(flat_rows, row_start, group_width, 1)
    partial_k = lax.dot_general(
        left_rows, flat_rows, (((0,), (0,)), ((), ())), preferred_element_type=F32
    )
    return lax.psum_scatter(partial_k, "aux", scatter_dimension=1, tiled=True)

TOP = 32000.0
FINE = 256.0


def kernel(
    aux_local, sizes, m_ref, metric_ref, out_ref, held, fit, left, early, acc, whole, kron_four, kron_two,
    rs_out, rs_in, z_in,
    gs, gr, zs, zr, fs, fr, rs, rr, cs, cr, ws, wr,
):
    z = lax.axis_index("aux")
    orb = lax.axis_index("orb")
    n_aux = m_ref.shape[0]
    parts = len(sizes)
    begins = [sum(sizes[:q]) for q in range(parts)]
    panel = acc.shape[1]
    pieces = 4
    rows = panel // pieces
    chip = orb // 2
    core = orb % 2
    x, y = chip % 2, chip // 2
    x_chip = chip + 1 - 2 * x
    y_chip = chip + 2 - 4 * y
    partner = orb + 1 - 2 * core
    other_chip = core * x_chip + (1 - core) * y_chip
    rs_peer = 2 * other_chip + core
    unused = core * (3 - 3 * y) + (1 - core) * (1 + x)
    odd_panel = 6 - unused - 3
    side = z // 2
    end = z % 3 == 0
    mate = z + 1 - 2 * (z % 2)
    far_end = 3 - 3 * side
    far_inner = 2 - side
    near_block = core * (1 + side) + (1 - core) * 3 * side
    far_block = 3 - near_block
    holder = near_block == z

    barrier = pltpu.get_barrier_semaphore()
    for d in (1, 2, 3):
        pl.semaphore_signal(
            barrier, inc=1, device_id={"aux": (z + d) % n_aux, "orb": orb}, device_id_type=MESH
        )
    for o in (partner, 2 * x_chip, 2 * x_chip + 1, 2 * y_chip, 2 * y_chip + 1):
        pl.semaphore_signal(barrier, inc=1, device_id={"aux": z, "orb": o}, device_id_type=MESH)
    pl.semaphore_wait(barrier, 8)

    def remote(src, dst, send, recv, a, o):
        return pltpu.make_async_remote_copy(
            src_ref=src, dst_ref=dst, send_sem=send, recv_sem=recv,
            device_id={"aux": a, "orb": o}, device_id_type=MESH,
        )

    def aligned(start, size, unit_of=128):
        return pl.ds(pl.multiple_of(start, unit_of), size)

    metric_rows = aligned(z * aux_local, aux_local, aux_local)
    gather = []
    for d in (1, 3, 2):
        copy = remote(metric_ref, whole.at[metric_rows], gs.at[d], gr.at[d], (z + d) % n_aux, orb)
        copy.start()
        gather.append(copy)

    def given_rows(q):
        return pl.ds(begins[q] * aux_local, sizes[q] * aux_local)

    def held_rows(source, q):
        unit = sizes[q] * aux_local
        return aligned(begins[q] * aux_local * n_aux + source * unit, unit, unit)

    MATE, FAR_END, FAR_INNER = 1, 2, 3
    sources = (z, mate, far_end, far_inner)

    def spread(r, q):
        there = sources[r]
        return remote(
            m_ref.at[there, given_rows(q)], held.at[0, held_rows(z, q)],
            zs.at[r * parts + q], zr.at[z * parts + q], there, orb,
        )

    @pl.when(end)
    def _():
        for r, q in (
            (FAR_END, 0), (FAR_END, 1), (FAR_END, 2), (FAR_END, 3), (MATE, 0), (FAR_INNER, 0),
            (MATE, 1), (FAR_INNER, 1), (MATE, 2), (MATE, 3), (FAR_INNER, 2), (FAR_INNER, 3),
        ):
            spread(r, q).start()

    @pl.when(jnp.logical_not(end))
    def _():
        for r, q in (
            (FAR_END, 0), (MATE, 0), (FAR_INNER, 0), (MATE, 1), (FAR_END, 1), (MATE, 2),
            (FAR_INNER, 1), (MATE, 3), (FAR_END, 2), (FAR_END, 3), (FAR_INNER, 2), (FAR_INNER, 3),
        ):
            spread(r, q).start()

    def recv_at(slot, r, q, k):
        return fr.at[((slot * 4 + r) * parts + q) * 2 + k]

    def shares(r, q):
        source = sources[r]
        at = held_rows(source, q)

        def cut(columns):
            if r == 0:
                return m_ref.at[z, given_rows(q), columns]
            return held.at[0, at, columns]

        jobs = [(partner, 1, pl.ds(0, 4 * panel), 0)]
        for o, slot, first, pair in (
            (2 * x_chip, 2 + core, 3 - 3 * x, 2 * x),
            (2 * y_chip + 1, 2 + core, 1 - y, 2 - y),
        ):
            jobs += [
                (o, slot, aligned(first * panel, panel), 0),
                (o, slot, aligned(pair * panel, 2 * panel), 1),
            ]
        return [
            remote(
                cut(columns), held.at[slot, at, columns],
                fs.at[(n * 4 + r) * parts + q], recv_at(slot, r, q, k), z, o,
            )
            for n, (o, slot, columns, k) in enumerate(jobs)
        ]

    def share(r, q):
        for copy in shares(r, q):
            copy.start()

    def arrive(r, q):
        here = held.at[0, held_rows(sources[r], q)]
        remote(here, here, zs.at[q], zr.at[sources[r] * parts + q], mate, orb).wait_recv()
        share(r, q)

    for q in range(parts):
        share(0, q)

    def slots_of(q):
        first = core * y + (1 - core) * 3 * x
        pair = core * (1 + y) + (1 - core) * 2 * (1 - x)
        one, two = aligned(first * panel, panel), aligned(pair * panel, 2 * panel)
        for r in range(4):
            at = held_rows(sources[r], q)
            for slot, k, columns in (
                (1, 0, pl.ds(0, 4 * panel)), (2, 0, one), (2, 1, two), (3, 0, one), (3, 1, two)
            ):
                here = held.at[slot, at, columns]
                remote(here, here, fs.at[0], recv_at(slot, r, q, k), z, partner).wait_recv()

    def build_kron(kron_ref):
        depth, wide = kron_ref.shape[0], whole.shape[1]
        unit = depth // n_aux

        def aux_of(r):
            return lax.div(r, unit) * aux_local + lax.rem(r, aux_local)

        def orbital_of(r):
            return lax.div(lax.rem(r, unit), aux_local)

        i32, bf16 = jnp.int32, kron_ref.dtype
        by_row = aux_of(lax.broadcasted_iota(i32, (wide, depth), 1))
        pick = jnp.where(by_row == lax.broadcasted_iota(i32, (wide, depth), 0), 1.0, 0.0)
        spread_cols = jnp.dot(whole[...], pick.astype(bf16), preferred_element_type=F32).astype(bf16)
        by_col = aux_of(lax.broadcasted_iota(i32, (depth, whole.shape[0]), 0))
        take = jnp.where(by_col == lax.broadcasted_iota(i32, (depth, whole.shape[0]), 1), 1.0, 0.0)
        both = jnp.dot(take.astype(bf16), spread_cols, preferred_element_type=F32)
        same = orbital_of(lax.broadcasted_iota(i32, (depth, depth), 0)) == orbital_of(
            lax.broadcasted_iota(i32, (depth, depth), 1)
        )
        kron_ref[...] = jnp.where(same, both, 0.0).astype(bf16)

    def place(p):
        return jnp.where(p == core, 0, jnp.where(p == 3 - core, 1, 2))

    def depth_of(q):
        return 4 * sizes[q] * aux_local * n_aux

    fit_at = (0, 0, 0, depth_of(2))

    def fit_part(q):
        slab = sizes[q] * aux_local * n_aux
        kron_ref = kron_four if sizes[q] == sizes[0] else kron_two
        base = begins[q] * aux_local * n_aux

        @pl.loop(0, 4)
        def _(slot):
            for n, p in enumerate((core, 3 - core, odd_panel)):
                fit[aligned(fit_at[q] + slot * slab, slab, slab), pl.ds(n * panel, panel)] = jnp.dot(
                    kron_ref[...], held[slot, pl.ds(base, slab), aligned(p * panel, panel)],
                    preferred_element_type=F32,
                ).astype(fit.dtype)

    def turn(p, q):
        chosen = other_chip if p else chip
        fitted = fit[pl.ds(fit_at[q], depth_of(q)), aligned(place(chosen) * panel, panel)]
        if p:
            early[:, pl.ds(0, depth_of(q))] = fitted.T
        else:
            left[:, pl.ds(fit_at[q], depth_of(q))] = fitted.T

    step = 2 * panel // 3
    far_tiles = ((1 - side) * step, (2 - side) * step)
    near_tile = side * 2 * step

    def contract(p, tile, q, begin):
        at = aligned(tile, step)
        if q is None:
            deep = fit_at[-1] + depth_of(parts - 1)
            more = jnp.dot(left[...], fit[pl.ds(0, deep), at], preferred_element_type=F32)
        elif p:
            more = jnp.dot(
                early[:, pl.ds(0, depth_of(q))], fit[pl.ds(fit_at[q], depth_of(q)), at],
                preferred_element_type=F32,
            )
        else:
            more = jnp.dot(
                left[:, pl.ds(fit_at[q], depth_of(q))], fit[pl.ds(fit_at[q], depth_of(q)), at],
                preferred_element_type=F32,
            )
        acc[p, :, at] = more if begin else acc[p, :, at] + more

    def contract_all(p, q, begin):
        @pl.loop(0, 3)
        def _(t):
            contract(p, t * step, q, begin)

    near, far = side, 1 - side
    strip = 32
    half = pieces // 2
    order = [(1 - core) * half + i for i in range(half)] + [core * half + i for i in range(half)]

    def block_at(block):
        return aligned(block * panel, panel)

    def quantize(p, block, h, target):
        at = block_at(block)

        def tops(t, top):
            some = acc[p, aligned(h * rows + t * strip, strip, strip), at]
            return jnp.maximum(top, jnp.max(jnp.abs(some).reshape(strip // 8, 8, panel), axis=0))

        top = lax.fori_loop(0, rows // strip, tops, jnp.zeros((8, panel), F32))
        top = jnp.maximum(jnp.max(top, axis=0, keepdims=True), 1e-30)
        level = jnp.ceil(jnp.log2(top) * FINE)
        scale = TOP * jnp.exp2(level * (-1.0 / FINE))

        @pl.loop(0, rows // strip)
        def _(t):
            some = acc[p, aligned(h * rows + t * strip, strip, strip), at]
            target[aligned(t * strip, strip, strip), :] = (
                jnp.round(some * scale).astype(jnp.int32).astype(jnp.int16)
            )

        target[pl.ds(rows, 16), :] = jnp.broadcast_to(
            level.astype(jnp.int32), (16, panel)
        ).astype(jnp.int16)

    def add_in(source, block, h):
        at = block_at(block)
        level = source[pl.ds(rows, 16), :].astype(F32)[:1]
        scale = jnp.exp2(level * (1.0 / FINE)) * (1.0 / TOP)

        @pl.loop(0, rows // strip)
        def _(t):
            here = aligned(h * rows + t * strip, strip, strip)
            some = source[aligned(t * strip, strip, strip), :].astype(F32)
            acc[0, here, at] = acc[0, here, at] + some * scale

    for q in range(parts):
        held[0, held_rows(z, q), :] = m_ref[z, given_rows(q), :]
    whole[metric_rows, :] = metric_ref[...]

    @pl.when(end)
    def _():
        for r, q in (
            (FAR_END, 0), (FAR_END, 1), (FAR_END, 2), (FAR_END, 3), (FAR_INNER, 0), (MATE, 0), (MATE, 1)
        ):
            arrive(r, q)

    @pl.when(jnp.logical_not(end))
    def _():
        for r, q in ((MATE, 0), (FAR_END, 0), (FAR_INNER, 0), (MATE, 1), (FAR_END, 1)):
            arrive(r, q)

    for copy in gather:
        copy.wait_recv()
    build_kron(kron_four)
    build_kron(kron_two)
    slots_of(0)
    fit_part(0)
    turn(0, 0)
    turn(1, 0)
    contract_all(1, 0, True)
    arrive(MATE, 2)
    contract_all(0, 0, True)
    arrive(MATE, 3)

    @pl.when(jnp.logical_not(end))
    def _():
        arrive(FAR_END, 2)
        arrive(FAR_END, 3)

    arrive(FAR_INNER, 1)
    slots_of(1)
    fit_part(1)
    turn(1, 1)
    turn(0, 1)
    contract_all(1, 1, False)
    arrive(FAR_INNER, 2)
    contract_all(0, 1, False)
    arrive(FAR_INNER, 3)
    slots_of(2)
    fit_part(2)
    turn(1, 2)
    contract_all(1, 2, False)
    slots_of(3)
    fit_part(3)
    turn(1, 3)

    def given(n):
        return remote(rs_out.at[n], rs_in.at[n], rs.at[n], rr.at[n], z, rs_peer)

    def give(block, n):
        quantize(1, block, order[n % pieces], rs_out.at[n])
        given(n).start()

    for tile in far_tiles:
        contract(1, tile, 3, False)
    give(far, 0)
    contract(1, near_tile, 3, False)
    give(near, pieces)
    for i in range(1, pieces):
        give(far, i)
        give(near, pieces + i)
    for q in range(2, parts):
        turn(0, q)
    for tile in (*far_tiles, near_tile):
        contract(0, tile, None, False)

    def along(n, into, there):
        return remote(rs_out.at[n], z_in.at[into], cs.at[n], cr.at[into], there, orb)

    inward = [along(i, i, mate) for i in range(pieces)]
    to_mate = [along(pieces + i, pieces + i, mate) for i in range(pieces)]
    across = [along(i, 2 * pieces + i, far_block) for i in range(pieces)]

    def pass_near(i):
        quantize(0, near, order[i], rs_out.at[pieces + i])
        to_mate[i].start()

    for i, h in enumerate(order):
        given(i).wait()
        add_in(rs_in.at[i], far, h)

        @pl.when(end)
        def _():
            quantize(0, far, h, rs_out.at[i])
            inward[i].start()

        @pl.when(jnp.logical_not(end))
        def _():
            inward[i].wait_recv()
            add_in(z_in.at[i], far, h)
            quantize(0, far, h, rs_out.at[i])
            across[i].start()

        given(pieces + i).wait()
        add_in(rs_in.at[pieces + i], near, h)

        @pl.when(jnp.logical_not(jnp.logical_or(holder, end)))
        def _():
            pass_near(i)

    @pl.when(jnp.logical_and(jnp.logical_not(holder), end))
    def _():
        for i in range(pieces):
            pass_near(i)

    own_at = block_at(near)

    def last(i):
        return remote(
            acc.at[0, aligned(order[i] * rows, rows, rows), own_at],
            out_ref.at[pl.ds(i * rows, rows)], ws.at[i], wr.at[i], z, partner,
        )

    @pl.when(holder)
    def _():
        for i, h in enumerate(order):
            to_mate[i].wait_recv()
            add_in(z_in.at[pieces + i], near, h)
        for i, h in enumerate(order):
            across[i].wait_recv()
            add_in(z_in.at[2 * pieces + i], near, h)
            if i < half:
                last(i).start()
            else:
                out_ref[pl.ds((i - half) * rows, rows), :] = acc[0, aligned(h * rows, rows, rows), own_at]
        for i in range(half):
            last(i).wait_send()

    @pl.when(jnp.logical_not(holder))
    def _():
        for i in range(half):
            last(i).wait_recv()
        for copy in to_mate:
            copy.wait_send()

    @pl.when(end)
    def _():
        for copy in inward:
            copy.wait_send()

    @pl.when(jnp.logical_not(end))
    def _():
        for copy in across:
            copy.wait_send()

    for copy in gather:
        copy.wait_send()
    for r in range(4):
        for q in range(parts):
            if r:
                spread(r, q).wait_send()
            for copy in shares(r, q):
                copy.wait_send()


def direct(half, metric, survive):
    aux_local, occ_local, ao = half.shape
    n_aux, n_orb = lax.axis_size("aux"), lax.axis_size("orb")
    part = occ_local // n_aux
    blocks = gated(half, survive).transpose(1, 0, 2).reshape(n_aux, part * aux_local, ao)
    n_fit = n_aux * aux_local
    width = -(-n_fit // 128) * 128
    metric = jnp.pad(metric, ((0, 0), (0, width - n_fit)))
    sizes = (part // 3, part // 3, part // 6, part // 6)
    parts = len(sizes)
    four, two = sizes[0] * n_fit, sizes[2] * n_fit
    late = 4 * four
    rows, panel = ao // n_orb, ao // n_aux
    dma = pltpu.SemaphoreType.DMA
    bf16, i16 = jnp.bfloat16, jnp.int16
    piece = (panel // 4 + 16, panel)
    return pl.pallas_call(
        functools.partial(kernel, aux_local, sizes),
        out_shape=jax.ShapeDtypeStruct((rows, panel), F32),
        in_specs=[pl.BlockSpec(memory_space=pltpu.VMEM)] * 2,
        out_specs=pl.BlockSpec(memory_space=pltpu.VMEM),
        scratch_shapes=[
            pltpu.VMEM((4, part * n_fit, ao), bf16),
            pltpu.VMEM((late, 3 * panel), bf16),
            pltpu.VMEM((panel, late), bf16),
            pltpu.VMEM((panel, 4 * four), bf16),
            pltpu.VMEM((2, panel, 2 * panel), F32),
            pltpu.VMEM((n_fit, width), bf16),
            pltpu.VMEM((four, four), bf16),
            pltpu.VMEM((two, two), bf16),
            pltpu.VMEM((8, *piece), i16),
            pltpu.VMEM((8, *piece), i16),
            pltpu.VMEM((12, *piece), i16),
            dma((4,)), dma((4,)),
            dma((4 * parts,)), dma((n_aux * parts,)),
            dma((20 * parts,)), dma((32 * parts,)),
            dma((8,)), dma((8,)),
            dma((8,)), dma((12,)),
            dma((2,)), dma((2,)),
        ],
        compiler_params=pltpu.CompilerParams(
            collective_id=0, has_side_effects=True, vmem_limit_bytes=66 * 1000 * 1000
        ),
    )(blocks, metric)


def solution(mesh):
    square = mesh.shape["aux"] == 4 and mesh.shape["orb"] == 8
    return jax.shard_map(
        direct if square else plain,
        mesh=mesh,
        in_specs=(P("aux", "orb", None), P("aux", None), P("aux", "orb", None)),
        out_specs=P("orb", "aux"),
        check_vma=False,
    )
```

```python
import functools

import jax
import jax.numpy as jnp
from jax import lax
from jax.experimental import pallas as pl
from jax.experimental.pallas import tpu as pltpu
from jax.sharding import PartitionSpec as P

MESH = pl.DeviceIdType.MESH
F32 = jnp.float32


def gated(half, survive):
    aux_local, occ_local, ao_count = half.shape
    blocks_aux, blocks_occ, blocks_ao = survive.shape
    gate = survive.astype(jnp.bfloat16)
    shaped = half.reshape(
        blocks_aux, aux_local, blocks_occ, occ_local // blocks_occ, blocks_ao, ao_count // blocks_ao
    )
    return (shaped * gate[:, None, :, None, :, None]).reshape(aux_local, occ_local, ao_count)


def plain(half, metric, survive):
    aux_local, occ_local, ao_count = half.shape
    portion = lax.all_gather(gated(half, survive), "aux", axis=0, tiled=True)
    fit_total = jnp.dot(metric, portion.reshape(portion.shape[0], -1), preferred_element_type=F32)
    fitted = fit_total.astype(jnp.bfloat16).reshape(aux_local, occ_local, ao_count)
    group_width = ao_count // lax.axis_size("orb")
    row_start = lax.axis_index("orb") * group_width
    flat_rows = lax.all_gather(fitted, "orb", axis=1, tiled=True).reshape(-1, ao_count)
    left_rows = lax.dynamic_slice_in_dim(flat_rows, row_start, group_width, 1)
    partial_k = lax.dot_general(
        left_rows, flat_rows, (((0,), (0,)), ((), ())), preferred_element_type=F32
    )
    return lax.psum_scatter(partial_k, "aux", scatter_dimension=1, tiled=True)

TOP = 32000.0
FINE = 256.0


def kernel(
    sizes, half_ref, metric_ref, survive_ref, out_ref, raw, m_ref, pick_ref, gate, metric_pad, held, fit, left, early, acc, whole, kron_four, kron_two,
    rs_out, rs_in, z_in,
    ls, gs, gr, zs, zr, fs, fr, rs, rr, cs, cr, ws, wr,
):
    z = lax.axis_index("aux")
    orb = lax.axis_index("orb")
    n_aux = m_ref.shape[0]
    aux_local, occ_local, ao = raw.shape
    parts = len(sizes)
    begins = [sum(sizes[:q]) for q in range(parts)]
    panel = acc.shape[1]
    unit_rows = panel // 8
    counts = [n * unit_rows for n in (1, 1, 2, 2, 1, 1)]
    starts = [n * unit_rows for n in (0, 1, 2, 0, 2, 3)]
    offsets = [n * unit_rows for n in (0, 1, 2, 4, 6, 7)]
    pieces = len(counts)
    chip = orb // 2
    core = orb % 2
    x, y = chip % 2, chip // 2
    x_chip = chip + 1 - 2 * x
    y_chip = chip + 2 - 4 * y
    partner = orb + 1 - 2 * core
    other_chip = core * x_chip + (1 - core) * y_chip
    rs_peer = 2 * other_chip + core
    unused = core * (3 - 3 * y) + (1 - core) * (1 + x)
    odd_panel = 6 - unused - 3
    side = z // 2
    end = z % 3 == 0
    mate = z + 1 - 2 * (z % 2)
    far_end = 3 - 3 * side
    far_inner = 2 - side
    near_block = core * (1 + side) + (1 - core) * 3 * side
    far_block = 3 - near_block
    holder = near_block == z

    barrier = pltpu.get_barrier_semaphore()
    for d in (1, 2, 3):
        pl.semaphore_signal(
            barrier, inc=1, device_id={"aux": (z + d) % n_aux, "orb": orb}, device_id_type=MESH
        )
    for o in (partner, 2 * x_chip, 2 * x_chip + 1, 2 * y_chip, 2 * y_chip + 1):
        pl.semaphore_signal(barrier, inc=1, device_id={"aux": z, "orb": o}, device_id_type=MESH)

    tiles = ls.shape[0]
    tile_width = ao // tiles
    loads = []
    for t in range(tiles):
        at = pl.ds(t * tile_width, tile_width)
        load = pltpu.make_async_copy(half_ref.at[:, :, at], raw.at[:, :, at], ls.at[t])
        load.start()
        loads.append(load)

    count = aux_local * occ_local
    out_row = lax.broadcasted_iota(jnp.int32, (count, count), 0)
    in_row = lax.broadcasted_iota(jnp.int32, (count, count), 1)
    wanted = lax.rem(out_row, aux_local) * occ_local + lax.div(out_row, aux_local)
    pick_ref[...] = jnp.where(in_row == wanted, 1.0, 0.0).astype(pick_ref.dtype)
    survived = survive_ref[...].astype(F32)
    ao_blocks = survive_ref.shape[1]
    block_width = ao // ao_blocks
    for b in range(ao_blocks):
        gate[:, pl.ds(b * block_width, block_width)] = jnp.broadcast_to(
            survived[:, b : b + 1], (gate.shape[0], block_width)
        )
    metric_pad[...] = jnp.zeros_like(metric_pad)
    metric_pad[:, pl.ds(0, metric_ref.shape[1])] = metric_ref[...]
    pl.semaphore_wait(barrier, 8)

    def remote(src, dst, send, recv, a, o):
        return pltpu.make_async_remote_copy(
            src_ref=src, dst_ref=dst, send_sem=send, recv_sem=recv,
            device_id={"aux": a, "orb": o}, device_id_type=MESH,
        )

    def aligned(start, size, unit_of=128):
        return pl.ds(pl.multiple_of(start, unit_of), size)

    metric_rows = aligned(z * aux_local, aux_local, aux_local)
    gather = []
    for d in (1, 3, 2):
        copy = remote(metric_pad, whole.at[metric_rows], gs.at[d], gr.at[d], (z + d) % n_aux, orb)
        copy.start()
        gather.append(copy)

    def given_rows(q):
        return pl.ds(begins[q] * aux_local, sizes[q] * aux_local)

    def held_rows(source, q):
        unit = sizes[q] * aux_local
        return aligned(begins[q] * aux_local * n_aux + source * unit, unit, unit)

    MATE, FAR_END, FAR_INNER = 1, 2, 3
    sources = (z, mate, far_end, far_inner)

    def spread(r, q):
        there = sources[r]
        return remote(
            m_ref.at[there, given_rows(q)], held.at[0, held_rows(z, q)],
            zs.at[r * parts + q], zr.at[z * parts + q], there, orb,
        )

    def sort_rows(pair, first):
        span = count // 2
        rows_at = pl.multiple_of(pair * span, span)
        for t in range(tiles):
            at = pl.ds(t * tile_width, tile_width)
            if first:
                loads[t].wait()
            sorted_rows = jnp.dot(
                pick_ref[pl.ds(rows_at, span), :], raw[:, :, at].reshape(count, tile_width),
                preferred_element_type=F32,
            )
            gated_rows = sorted_rows * gate[pl.ds(pair, 1), at]
            m_ref[pl.ds(2 * pair, 2), :, at] = gated_rows.astype(m_ref.dtype).reshape(
                2, span // 2, tile_width
            )

    sort_rows(1 - side, True)

    @pl.when(end)
    def _():
        for q in range(parts):
            spread(FAR_END, q).start()

    @pl.when(jnp.logical_not(end))
    def _():
        for r, q in (
            (FAR_END, 0), (FAR_END, 1), (FAR_INNER, 0), (FAR_END, 2), (FAR_END, 3),
            (FAR_END, 4), (FAR_INNER, 1), (FAR_INNER, 2), (FAR_INNER, 3), (FAR_INNER, 4),
        ):
            spread(r, q).start()

    sort_rows(side, False)

    @pl.when(end)
    def _():
        for r, q in (
            (MATE, 0), (MATE, 1), (FAR_INNER, 0), (FAR_INNER, 1), (MATE, 2),
            (MATE, 3), (MATE, 4), (FAR_INNER, 2), (FAR_INNER, 3), (FAR_INNER, 4),
        ):
            spread(r, q).start()

    @pl.when(jnp.logical_not(end))
    def _():
        for q in range(parts):
            spread(MATE, q).start()

    def recv_at(slot, r, q, k):
        return fr.at[(((slot - 1) * 4 + r) * parts + q) * 2 + k]

    def shares(r, q):
        source = sources[r]
        at = held_rows(source, q)

        def cut(columns):
            if r == 0:
                return m_ref.at[z, given_rows(q), columns]
            return held.at[0, at, columns]

        jobs = [(partner, 1, pl.ds(0, 4 * panel), 0)]
        for o, slot, first, pair in (
            (2 * x_chip, 2 + core, 3 - 3 * x, 2 * x),
            (2 * y_chip + 1, 2 + core, 1 - y, 2 - y),
        ):
            jobs += [
                (o, slot, aligned(first * panel, panel), 0),
                (o, slot, aligned(pair * panel, 2 * panel), 1),
            ]
        return [
            remote(
                cut(columns), held.at[slot, at, columns],
                fs.at[(n * 4 + r) * parts + q], recv_at(slot, r, q, k), z, o,
            )
            for n, (o, slot, columns, k) in enumerate(jobs)
        ]

    def share(r, q):
        for copy in shares(r, q):
            copy.start()

    def arrive(r, q):
        here = held.at[0, held_rows(sources[r], q)]
        remote(here, here, zs.at[q], zr.at[sources[r] * parts + q], mate, orb).wait_recv()
        share(r, q)

    for q in range(parts):
        share(0, q)

    def slots_of(q):
        first = core * y + (1 - core) * 3 * x
        pair = core * (1 + y) + (1 - core) * 2 * (1 - x)
        one, two = aligned(first * panel, panel), aligned(pair * panel, 2 * panel)
        for r in range(4):
            at = held_rows(sources[r], q)
            for slot, k, columns in (
                (1, 0, pl.ds(0, 4 * panel)), (2, 0, one), (2, 1, two), (3, 0, one), (3, 1, two)
            ):
                here = held.at[slot, at, columns]
                remote(here, here, fs.at[0], recv_at(slot, r, q, k), z, partner).wait_recv()

    def build_kron(kron_ref):
        depth, wide = kron_ref.shape[0], whole.shape[1]
        unit = depth // n_aux

        def aux_of(r):
            return lax.div(r, unit) * aux_local + lax.rem(r, aux_local)

        def orbital_of(r):
            return lax.div(lax.rem(r, unit), aux_local)

        i32, bf16 = jnp.int32, kron_ref.dtype
        by_row = aux_of(lax.broadcasted_iota(i32, (wide, depth), 1))
        pick = jnp.where(by_row == lax.broadcasted_iota(i32, (wide, depth), 0), 1.0, 0.0)
        spread_cols = jnp.dot(whole[...], pick.astype(bf16), preferred_element_type=F32).astype(bf16)
        by_col = aux_of(lax.broadcasted_iota(i32, (depth, whole.shape[0]), 0))
        take = jnp.where(by_col == lax.broadcasted_iota(i32, (depth, whole.shape[0]), 1), 1.0, 0.0)
        both = jnp.dot(take.astype(bf16), spread_cols, preferred_element_type=F32)
        same = orbital_of(lax.broadcasted_iota(i32, (depth, depth), 0)) == orbital_of(
            lax.broadcasted_iota(i32, (depth, depth), 1)
        )
        kron_ref[...] = jnp.where(same, both, 0.0).astype(bf16)

    def place(p):
        return jnp.where(p == core, 0, jnp.where(p == 3 - core, 1, 2))

    def depth_of(q):
        return 4 * sizes[q] * aux_local * n_aux

    fit_at = (0, 0, 0, depth_of(2), 2 * depth_of(2))

    def fit_part(q):
        slab = sizes[q] * aux_local * n_aux
        kron_ref = kron_four if sizes[q] == sizes[0] else kron_two
        base = begins[q] * aux_local * n_aux

        @pl.loop(0, 4)
        def _(slot):
            for n, p in enumerate((core, 3 - core, odd_panel)):
                fit[aligned(fit_at[q] + slot * slab, slab, slab), pl.ds(n * panel, panel)] = jnp.dot(
                    kron_ref[...], held[slot, pl.ds(base, slab), aligned(p * panel, panel)],
                    preferred_element_type=F32,
                ).astype(fit.dtype)

    def turn(p, q):
        chosen = other_chip if p else chip
        fitted = fit[pl.ds(fit_at[q], depth_of(q)), aligned(place(chosen) * panel, panel)]
        if p:
            early[:, pl.ds(0, depth_of(q))] = fitted.T
        else:
            left[:, pl.ds(fit_at[q], depth_of(q))] = fitted.T

    step = 2 * panel // 3
    mixed = jnp.logical_not(jnp.logical_or(end, holder))
    far_edge, near_edge = (1 - side) * 2 * step, side * 2 * step

    def contract(p, tile, q, begin):
        at = aligned(tile, step)
        if q is None:
            deep = fit_at[-1] + depth_of(parts - 1)
            more = jnp.dot(left[...], fit[pl.ds(0, deep), at], preferred_element_type=F32)
        elif p:
            more = jnp.dot(
                early[:, pl.ds(0, depth_of(q))], fit[pl.ds(fit_at[q], depth_of(q)), at],
                preferred_element_type=F32,
            )
        else:
            more = jnp.dot(
                left[:, pl.ds(fit_at[q], depth_of(q))], fit[pl.ds(fit_at[q], depth_of(q)), at],
                preferred_element_type=F32,
            )
        acc[p, :, at] = more if begin else acc[p, :, at] + more

    def contract_all(p, q, begin):
        @pl.loop(0, 3)
        def _(t):
            contract(p, t * step, q, begin)

    near, far = side, 1 - side
    strip = 32
    half = pieces // 2
    sides_of = [1 - core] * half + [core] * half
    order = [sides_of[i] * 4 * unit_rows + starts[i] for i in range(pieces)]
    FAR, NEAR, MORE = 0, 1, 2

    def block_at(block):
        return aligned(block * panel, panel)

    def tops_of(p, block):
        at = block_at(block)

        def tops(t, top):
            some = acc[p, aligned(t * strip, strip, strip), at]
            return jnp.maximum(top, jnp.max(jnp.abs(some).reshape(strip // 8, 8, panel), axis=0))

        top = lax.fori_loop(0, panel // strip, tops, jnp.zeros((8, panel), F32))
        return jnp.max(top, axis=0, keepdims=True)

    def level_of(top):
        return jnp.ceil(jnp.log2(jnp.maximum(top, 1e-30)) * FINE)

    def rows_of(i):
        if i == 0:
            return pl.ds(0, 16 + counts[0])
        return pl.ds(16 + offsets[i], counts[i])

    def bound_of(source):
        return jnp.exp2(source[pl.ds(0, 16), :].astype(F32)[:1] * (1.0 / FINE))

    def quantize(p, block, i, level, target):
        at = block_at(block)
        scale = TOP * jnp.exp2(level * (-1.0 / FINE))

        @pl.loop(0, counts[i] // strip)
        def _(t):
            some = acc[p, aligned(order[i] + t * strip, strip, strip), at]
            target[aligned(16 + offsets[i] + t * strip, strip, 16), :] = (
                jnp.round(some * scale).astype(jnp.int32).astype(jnp.int16)
            )

        if i == 0:
            target[pl.ds(0, 16), :] = jnp.broadcast_to(
                level.astype(jnp.int32), (16, panel)
            ).astype(jnp.int16)

    def add_in(source, bound, block, i):
        at = block_at(block)
        scale = bound * (1.0 / TOP)

        @pl.loop(0, counts[i] // strip)
        def _(t):
            here = aligned(order[i] + t * strip, strip, strip)
            some = source[aligned(16 + offsets[i] + t * strip, strip, 16), :].astype(F32)
            acc[0, here, at] = acc[0, here, at] + some * scale

    for q in range(parts):
        held[0, held_rows(z, q), :] = m_ref[z, given_rows(q), :]
    whole[metric_rows, :] = metric_pad[...]

    @pl.when(end)
    def _():
        for r, q in (
            (FAR_END, 0), (FAR_END, 1), (FAR_END, 2), (FAR_END, 3), (FAR_END, 4),
            (FAR_INNER, 0), (FAR_INNER, 1), (MATE, 0), (MATE, 1),
        ):
            arrive(r, q)

    @pl.when(jnp.logical_not(end))
    def _():
        for r, q in (
            (MATE, 0), (MATE, 1), (FAR_END, 0), (FAR_END, 1), (MATE, 2), (FAR_INNER, 0),
            (MATE, 3), (MATE, 4),
        ):
            arrive(r, q)

    for copy in gather:
        copy.wait_recv()
    build_kron(kron_four)
    build_kron(kron_two)
    slots_of(0)
    fit_part(0)
    turn(0, 0)
    turn(1, 0)
    contract_all(1, 0, True)
    contract_all(0, 0, True)

    @pl.when(end)
    def _():
        for q in (2, 3, 4):
            arrive(MATE, q)

    @pl.when(jnp.logical_not(end))
    def _():
        for q in (2, 3, 4):
            arrive(FAR_END, q)
        arrive(FAR_INNER, 1)

    arrive(FAR_INNER, 2)
    slots_of(1)
    fit_part(1)
    turn(1, 1)
    turn(0, 1)
    contract_all(1, 1, False)
    arrive(FAR_INNER, 3)
    contract_all(0, 1, False)
    slots_of(2)
    fit_part(2)
    turn(1, 2)
    arrive(FAR_INNER, 4)
    contract_all(1, 2, False)
    slots_of(3)
    fit_part(3)
    turn(1, 3)
    contract_all(1, 3, False)
    slots_of(4)
    fit_part(4)
    turn(1, 4)

    def given(k, i):
        at, n = rows_of(i), k * pieces + i
        return remote(rs_out.at[k, at], rs_in.at[k, at], rs.at[n], rr.at[n], z, rs_peer)

    def give(k, level, i):
        quantize(1, (far, near)[k], i, level, rs_out.at[k])
        given(k, i).start()

    contract(1, far_edge, 4, False)
    contract(1, step, 4, False)
    far_level = level_of(tops_of(1, far))
    F, N = FAR, NEAR
    hold = jnp.logical_and(holder, jnp.logical_not(end))
    in_order = tuple((k, i) for k in (F, N) for i in range(pieces))
    mixed_order = (
        (F, 0), (F, 1), (F, 2), (N, 0), (F, 3), (N, 1), (F, 4), (N, 2), (N, 3), (F, 5), (N, 4), (N, 5),
    )
    hold_order = (
        (F, 0), (F, 1), (N, 0), (N, 1), (N, 2), (F, 2), (N, 3), (F, 3), (F, 4), (F, 5), (N, 4), (N, 5),
    )
    for i in range(2):
        give(FAR, far_level, i)

    @pl.when(mixed)
    def _():
        give(FAR, far_level, 2)

    @pl.when(end)
    def _():
        for i in range(2, pieces):
            give(FAR, far_level, i)

    for q in range(2, parts):
        turn(0, q)
    contract(0, far_edge, None, False)
    contract(0, step, None, False)
    far_top = tops_of(0, far)

    def along(k, i, into, there):
        at, n = rows_of(i), k * pieces + i
        return remote(
            rs_out.at[k, at], z_in.at[into, at], cs.at[n], cr.at[into * pieces + i], there, orb
        )

    def inward(i):
        return along(FAR, i, FAR, mate)

    def to_mate(i):
        return along(NEAR, i, NEAR, mate)

    def across(i):
        return along(FAR, i, MORE, far_inner)

    def near_given(i):
        given(NEAR, i).wait()
        add_in(rs_in.at[NEAR], bound_of(rs_in.at[NEAR]), near, i)

    def far_given(i):
        given(FAR, i).wait()
        add_in(rs_in.at[FAR], bound_of(rs_in.at[FAR]), far, i)

    def far_to_mate(i):
        far_given(i)
        quantize(0, far, i, level_of(far_top + bound_of(rs_in.at[FAR])), rs_out.at[FAR])
        inward(i).start()

    def far_across(i):
        far_given(i)
        inward(i).wait_recv()
        more = bound_of(z_in.at[FAR])
        add_in(z_in.at[FAR], more, far, i)
        total = far_top + bound_of(rs_in.at[FAR]) + more
        quantize(0, far, i, level_of(total), rs_out.at[FAR])
        across(i).start()

    own_at = block_at(near)

    def last(i):
        return remote(
            acc.at[0, aligned(order[i], counts[i], counts[i]), own_at],
            out_ref.at[pl.ds(starts[i], counts[i])], ws.at[i], wr.at[i], z, partner,
        )

    def settle(i):
        return pltpu.make_async_copy(
            acc.at[0, aligned(order[i], counts[i], counts[i]), own_at],
            out_ref.at[pl.ds(starts[i], counts[i])], ws.at[i],
        )

    @pl.when(end)
    def _():
        far_to_mate(0)

    @pl.when(jnp.logical_not(end))
    def _():
        far_across(0)

    contract(1, near_edge, 4, False)
    near_level = level_of(tops_of(1, near))
    def give_rest(sequence):
        for k, i in sequence:
            give(k, (far_level, near_level)[k], i)

    @pl.when(mixed)
    def _():
        give_rest(mixed_order[3:])

    @pl.when(hold)
    def _():
        give_rest(hold_order[2:])

    @pl.when(end)
    def _():
        give_rest(in_order[pieces:])

    contract(0, near_edge, None, False)
    near_top = tops_of(0, near)

    def near_pass(i, combined):
        near_given(i)
        total = near_top + bound_of(rs_in.at[NEAR])
        if combined:
            across(i).wait_recv()
            more = bound_of(z_in.at[MORE])
            add_in(z_in.at[MORE], more, near, i)
            total = total + more
        quantize(0, near, i, level_of(total), rs_out.at[NEAR])
        to_mate(i).start()

    @pl.when(mixed)
    def _():
        for k, i in mixed_order[1:]:
            if k == F:
                far_across(i)
            else:
                near_pass(i, True)

    @pl.when(end)
    def _():
        for i in range(1, pieces):
            far_to_mate(i)

    @pl.when(hold)
    def _():
        for k, i in hold_order[1:]:
            if k == F:
                far_across(i)
            else:
                near_given(i)

    @pl.when(jnp.logical_and(end, jnp.logical_not(holder)))
    def _():
        for i in range(pieces):
            near_pass(i, False)

    for copy in gather:
        copy.wait_send()
    for r in range(4):
        for q in range(parts):
            if r:
                spread(r, q).wait_send()
            for copy in shares(r, q):
                copy.wait_send()

    def finish(crossed):
        for i in range(pieces):
            to_mate(i).wait_recv()
            add_in(z_in.at[NEAR], bound_of(z_in.at[NEAR]), near, i)
            if crossed:
                across(i).wait_recv()
                add_in(z_in.at[MORE], bound_of(z_in.at[MORE]), near, i)
            if i < half:
                last(i).start()
            else:
                settle(i).start()
        for i in range(half):
            last(i).wait_send()
            settle(half + i).wait()

    @pl.when(jnp.logical_and(holder, end))
    def _():
        for i in range(pieces):
            near_given(i)
        finish(False)

    @pl.when(hold)
    def _():
        finish(True)

    @pl.when(jnp.logical_not(holder))
    def _():
        for i in range(half):
            last(i).wait_recv()

    for i in range(pieces):
        inward(i).wait_send()

    @pl.when(jnp.logical_not(holder))
    def _():
        for i in range(pieces):
            to_mate(i).wait_send()


def direct(half, metric, survive):
    aux_local, occ_local, ao = half.shape
    n_aux, n_orb = lax.axis_size("aux"), lax.axis_size("orb")
    part = occ_local // n_aux
    if survive.shape[:2] != (1, 2) or part % 6:
        return plain(half, metric, survive)
    survive = survive.reshape(survive.shape[1:])
    n_fit = n_aux * aux_local
    width = -(-n_fit // 128) * 128
    sizes = (part // 3,) + (part // 6,) * 4
    parts = len(sizes)
    four, two = sizes[0] * n_fit, sizes[1] * n_fit
    late = 12 * two
    rows, panel = ao // n_orb, ao // n_aux
    dma = pltpu.SemaphoreType.DMA
    bf16, i16 = jnp.bfloat16, jnp.int16
    block = (panel + 16, panel)
    return pl.pallas_call(
        functools.partial(kernel, sizes),
        out_shape=jax.ShapeDtypeStruct((rows, panel), F32),
        in_specs=[pl.BlockSpec(memory_space=pl.ANY)] + [pl.BlockSpec(memory_space=pltpu.VMEM)] * 2,
        out_specs=pl.BlockSpec(memory_space=pl.ANY),
        scratch_shapes=[
            pltpu.VMEM((aux_local, occ_local, ao), bf16),
            pltpu.VMEM((n_aux, part * aux_local, ao), bf16),
            pltpu.VMEM((aux_local * occ_local, aux_local * occ_local), bf16),
            pltpu.VMEM((survive.shape[0], ao), F32),
            pltpu.VMEM((aux_local, width), bf16),
            pltpu.VMEM((4, part * n_fit, ao), bf16),
            pltpu.VMEM((late, 3 * panel), bf16),
            pltpu.VMEM((panel, late), bf16),
            pltpu.VMEM((panel, 4 * four), bf16),
            pltpu.VMEM((2, panel, 2 * panel), F32),
            pltpu.VMEM((n_fit, width), bf16),
            pltpu.VMEM((four, four), bf16),
            pltpu.VMEM((two, two), bf16),
            pltpu.VMEM((2, *block), i16),
            pltpu.VMEM((2, *block), i16),
            pltpu.VMEM((3, *block), i16),
            dma((6,)),
            dma((4,)), dma((4,)),
            dma((4 * parts,)), dma((n_aux * parts,)),
            dma((20 * parts,)), dma((24 * parts,)),
            dma((12,)), dma((12,)),
            dma((12,)), dma((18,)),
            dma((6,)), dma((3,)),
        ],
        compiler_params=pltpu.CompilerParams(
            collective_id=0, has_side_effects=True, vmem_limit_bytes=66 * 1000 * 1000
        ),
    )(half, metric, survive)


def solution(mesh):
    square = mesh.shape["aux"] == 4 and mesh.shape["orb"] == 8
    return jax.shard_map(
        direct if square else plain,
        mesh=mesh,
        in_specs=(P("aux", "orb", None), P("aux", None), P("aux", "orb", None)),
        out_specs=P("orb", "aux"),
        check_vma=False,
    )
```

```python
import functools

import jax
import jax.numpy as jnp
from jax import lax
from jax.experimental import pallas as pl
from jax.experimental.pallas import tpu as pltpu
from jax.sharding import PartitionSpec as P

MESH = pl.DeviceIdType.MESH
F32 = jnp.float32


def gated(half, survive):
    aux_local, occ_local, ao_count = half.shape
    blocks_aux, blocks_occ, blocks_ao = survive.shape
    gate = survive.astype(jnp.bfloat16)
    shaped = half.reshape(
        blocks_aux, aux_local, blocks_occ, occ_local // blocks_occ, blocks_ao, ao_count // blocks_ao
    )
    return (shaped * gate[:, None, :, None, :, None]).reshape(aux_local, occ_local, ao_count)


def plain(half, metric, survive):
    aux_local, occ_local, ao_count = half.shape
    portion = lax.all_gather(gated(half, survive), "aux", axis=0, tiled=True)
    fit_total = jnp.dot(metric, portion.reshape(portion.shape[0], -1), preferred_element_type=F32)
    fitted = fit_total.astype(jnp.bfloat16).reshape(aux_local, occ_local, ao_count)
    group_width = ao_count // lax.axis_size("orb")
    row_start = lax.axis_index("orb") * group_width
    flat_rows = lax.all_gather(fitted, "orb", axis=1, tiled=True).reshape(-1, ao_count)
    left_rows = lax.dynamic_slice_in_dim(flat_rows, row_start, group_width, 1)
    partial_k = lax.dot_general(
        left_rows, flat_rows, (((0,), (0,)), ((), ())), preferred_element_type=F32
    )
    return lax.psum_scatter(partial_k, "aux", scatter_dimension=1, tiled=True)

TOP = 32000.0
FINE = 256.0


def kernel(
    sizes, half_ref, metric_ref, survive_ref, out_ref, raw, m_ref, pick_ref, gate, metric_pad, held, fit, left, early, acc, whole, kron_four, kron_two,
    rs_out, rs_in, z_in,
    ls, gs, gr, zs, zr, fs, fr, rs, rr, cs, cr, ws, wr,
):
    z = lax.axis_index("aux")
    orb = lax.axis_index("orb")
    n_aux = m_ref.shape[0]
    aux_local, occ_local, ao = raw.shape
    parts = len(sizes)
    begins = [sum(sizes[:q]) for q in range(parts)]
    panel = acc.shape[1]
    unit_rows = panel // 8
    counts = [n * unit_rows for n in (1, 1, 2, 2, 1, 1)]
    starts = [n * unit_rows for n in (0, 1, 2, 0, 2, 3)]
    offsets = [n * unit_rows for n in (0, 1, 2, 4, 6, 7)]
    pieces = len(counts)
    chip = orb // 2
    core = orb % 2
    x, y = chip % 2, chip // 2
    x_chip = chip + 1 - 2 * x
    y_chip = chip + 2 - 4 * y
    partner = orb + 1 - 2 * core
    other_chip = core * x_chip + (1 - core) * y_chip
    rs_peer = 2 * other_chip + core
    unused = core * (3 - 3 * y) + (1 - core) * (1 + x)
    odd_panel = 6 - unused - 3
    side = z // 2
    end = z % 3 == 0
    mate = z + 1 - 2 * (z % 2)
    far_end = 3 - 3 * side
    far_inner = 2 - side
    near_block = core * (1 + side) + (1 - core) * 3 * side
    far_block = 3 - near_block
    holder = near_block == z

    barrier = pltpu.get_barrier_semaphore()
    for d in (1, 2, 3):
        pl.semaphore_signal(
            barrier, inc=1, device_id={"aux": (z + d) % n_aux, "orb": orb}, device_id_type=MESH
        )
    for o in (partner, 2 * x_chip, 2 * x_chip + 1, 2 * y_chip, 2 * y_chip + 1):
        pl.semaphore_signal(barrier, inc=1, device_id={"aux": z, "orb": o}, device_id_type=MESH)

    tiles = ls.shape[0]
    tile_width = ao // tiles
    loads = []
    for t in range(tiles):
        at = pl.ds(t * tile_width, tile_width)
        load = pltpu.make_async_copy(half_ref.at[:, :, at], raw.at[:, :, at], ls.at[t])
        load.start()
        loads.append(load)

    count = aux_local * occ_local
    out_row = lax.broadcasted_iota(jnp.int32, (count, count), 0)
    in_row = lax.broadcasted_iota(jnp.int32, (count, count), 1)
    wanted = lax.rem(out_row, aux_local) * occ_local + lax.div(out_row, aux_local)
    pick_ref[...] = jnp.where(in_row == wanted, 1.0, 0.0).astype(pick_ref.dtype)
    survived = survive_ref[...].astype(F32)
    ao_blocks = survive_ref.shape[1]
    block_width = ao // ao_blocks
    for b in range(ao_blocks):
        gate[:, pl.ds(b * block_width, block_width)] = jnp.broadcast_to(
            survived[:, b : b + 1], (gate.shape[0], block_width)
        )
    metric_pad[...] = jnp.zeros_like(metric_pad)
    metric_pad[:, pl.ds(0, metric_ref.shape[1])] = metric_ref[...]

    def remote(src, dst, send, recv, a, o):
        return pltpu.make_async_remote_copy(
            src_ref=src, dst_ref=dst, send_sem=send, recv_sem=recv,
            device_id={"aux": a, "orb": o}, device_id_type=MESH,
        )

    def aligned(start, size, unit_of=128):
        return pl.ds(pl.multiple_of(start, unit_of), size)

    def given_rows(q):
        return pl.ds(begins[q] * aux_local, sizes[q] * aux_local)

    def held_rows(source, q):
        unit = sizes[q] * aux_local
        return aligned(begins[q] * aux_local * n_aux + source * unit, unit, unit)

    MATE, FAR_END, FAR_INNER = 1, 2, 3
    sources = (z, mate, far_end, far_inner)

    def spread(r, q):
        there = sources[r]
        return remote(
            m_ref.at[there, given_rows(q)], held.at[0, held_rows(z, q)],
            zs.at[r * parts + q], zr.at[z * parts + q], there, orb,
        )

    def sort_rows(pair, first):
        span = count // 2
        rows_at = pl.multiple_of(pair * span, span)
        for t in range(tiles):
            at = pl.ds(t * tile_width, tile_width)
            if first:
                loads[t].wait()
            sorted_rows = jnp.dot(
                pick_ref[pl.ds(rows_at, span), :], raw[:, :, at].reshape(count, tile_width),
                preferred_element_type=F32,
            )
            gated_rows = sorted_rows * gate[pl.ds(pair, 1), at]
            m_ref[pl.ds(2 * pair, 2), :, at] = gated_rows.astype(m_ref.dtype).reshape(
                2, span // 2, tile_width
            )

    sort_rows(1 - side, True)
    pl.semaphore_wait(barrier, 8)

    metric_rows = aligned(z * aux_local, aux_local, aux_local)
    gather = []
    for d in (1, 3, 2):
        copy = remote(metric_pad, whole.at[metric_rows], gs.at[d], gr.at[d], (z + d) % n_aux, orb)
        copy.start()
        gather.append(copy)

    @pl.when(end)
    def _():
        for q in range(parts):
            spread(FAR_END, q).start()

    @pl.when(jnp.logical_not(end))
    def _():
        for r, q in (
            (FAR_END, 0), (FAR_END, 1), (FAR_INNER, 0), (FAR_INNER, 1), (FAR_END, 2),
            (FAR_END, 3), (FAR_END, 4), (FAR_INNER, 2), (FAR_INNER, 3), (FAR_INNER, 4),
        ):
            spread(r, q).start()

    sort_rows(side, False)

    @pl.when(end)
    def _():
        for r, q in (
            (MATE, 0), (MATE, 1), (FAR_INNER, 0), (FAR_INNER, 1), (MATE, 2),
            (MATE, 3), (MATE, 4), (FAR_INNER, 2), (FAR_INNER, 3), (FAR_INNER, 4),
        ):
            spread(r, q).start()

    @pl.when(jnp.logical_not(end))
    def _():
        for q in range(parts):
            spread(MATE, q).start()

    def recv_at(slot, r, q, k):
        return fr.at[(((slot - 1) * 4 + r) * parts + q) * 2 + k]

    def shares(r, q):
        source = sources[r]
        at = held_rows(source, q)

        def cut(columns):
            if r == 0:
                return m_ref.at[z, given_rows(q), columns]
            return held.at[0, at, columns]

        jobs = [(partner, 1, pl.ds(0, 4 * panel), 0)]
        for o, slot, first, pair in (
            (2 * x_chip, 2 + core, 3 - 3 * x, 2 * x),
            (2 * y_chip + 1, 2 + core, 1 - y, 2 - y),
        ):
            jobs += [
                (o, slot, aligned(first * panel, panel), 0),
                (o, slot, aligned(pair * panel, 2 * panel), 1),
            ]
        return [
            remote(
                cut(columns), held.at[slot, at, columns],
                fs.at[(n * 4 + r) * parts + q], recv_at(slot, r, q, k), z, o,
            )
            for n, (o, slot, columns, k) in enumerate(jobs)
        ]

    def share(r, q):
        for copy in shares(r, q):
            copy.start()

    def arrive(r, q):
        here = held.at[0, held_rows(sources[r], q)]
        remote(here, here, zs.at[q], zr.at[sources[r] * parts + q], mate, orb).wait_recv()
        share(r, q)

    for q in range(parts):
        share(0, q)

    def slots_of(q):
        first = core * y + (1 - core) * 3 * x
        pair = core * (1 + y) + (1 - core) * 2 * (1 - x)
        one, two = aligned(first * panel, panel), aligned(pair * panel, 2 * panel)
        for r in range(4):
            at = held_rows(sources[r], q)
            for slot, k, columns in (
                (1, 0, pl.ds(0, 4 * panel)), (2, 0, one), (2, 1, two), (3, 0, one), (3, 1, two)
            ):
                here = held.at[slot, at, columns]
                remote(here, here, fs.at[0], recv_at(slot, r, q, k), z, partner).wait_recv()

    def build_kron(kron_ref):
        depth, wide = kron_ref.shape[0], whole.shape[1]
        unit = depth // n_aux

        def aux_of(r):
            return lax.div(r, unit) * aux_local + lax.rem(r, aux_local)

        def orbital_of(r):
            return lax.div(lax.rem(r, unit), aux_local)

        i32, bf16 = jnp.int32, kron_ref.dtype
        by_row = aux_of(lax.broadcasted_iota(i32, (wide, depth), 1))
        pick = jnp.where(by_row == lax.broadcasted_iota(i32, (wide, depth), 0), 1.0, 0.0)
        spread_cols = jnp.dot(whole[...], pick.astype(bf16), preferred_element_type=F32).astype(bf16)
        by_col = aux_of(lax.broadcasted_iota(i32, (depth, whole.shape[0]), 0))
        take = jnp.where(by_col == lax.broadcasted_iota(i32, (depth, whole.shape[0]), 1), 1.0, 0.0)
        both = jnp.dot(take.astype(bf16), spread_cols, preferred_element_type=F32)
        same = orbital_of(lax.broadcasted_iota(i32, (depth, depth), 0)) == orbital_of(
            lax.broadcasted_iota(i32, (depth, depth), 1)
        )
        kron_ref[...] = jnp.where(same, both, 0.0).astype(bf16)

    def place(p):
        return jnp.where(p == core, 0, jnp.where(p == 3 - core, 1, 2))

    def depth_of(q):
        return 4 * sizes[q] * aux_local * n_aux

    fit_at = (0, 0, 0, depth_of(2), 2 * depth_of(2))

    def fit_part(q):
        slab = sizes[q] * aux_local * n_aux
        kron_ref = kron_four if sizes[q] == sizes[0] else kron_two
        base = begins[q] * aux_local * n_aux

        @pl.loop(0, 4)
        def _(slot):
            for n, p in enumerate((core, 3 - core, odd_panel)):
                fit[aligned(fit_at[q] + slot * slab, slab, slab), pl.ds(n * panel, panel)] = jnp.dot(
                    kron_ref[...], held[slot, pl.ds(base, slab), aligned(p * panel, panel)],
                    preferred_element_type=F32,
                ).astype(fit.dtype)

    def turn(p, q):
        chosen = other_chip if p else chip
        fitted = fit[pl.ds(fit_at[q], depth_of(q)), aligned(place(chosen) * panel, panel)]
        if p:
            early[:, pl.ds(0, depth_of(q))] = fitted.T
        else:
            left[:, pl.ds(fit_at[q], depth_of(q))] = fitted.T

    step = 2 * panel // 3
    mixed = jnp.logical_not(jnp.logical_or(end, holder))
    far_edge, near_edge = (1 - side) * 2 * step, side * 2 * step

    def contract(p, tile, q, begin):
        at = aligned(tile, step)
        if q is None:
            late = pl.ds(fit_at[begin], fit_at[-1] + depth_of(parts - 1) - fit_at[begin])
            more = jnp.dot(left[:, late], fit[late, at], preferred_element_type=F32)
        elif p:
            more = jnp.dot(
                early[:, pl.ds(0, depth_of(q))], fit[pl.ds(fit_at[q], depth_of(q)), at],
                preferred_element_type=F32,
            )
        else:
            more = jnp.dot(
                left[:, pl.ds(fit_at[q], depth_of(q))], fit[pl.ds(fit_at[q], depth_of(q)), at],
                preferred_element_type=F32,
            )
        acc[p, :, at] = more if begin is True else acc[p, :, at] + more

    def contract_all(p, q, begin):
        @pl.loop(0, 3)
        def _(t):
            contract(p, t * step, q, begin)

    near, far = side, 1 - side
    strip = 32
    half = pieces // 2
    sides_of = [1 - core] * half + [core] * half
    order = [sides_of[i] * 4 * unit_rows + starts[i] for i in range(pieces)]
    FAR, NEAR, MORE = 0, 1, 2

    def block_at(block):
        return aligned(block * panel, panel)

    def tops_of(p, block):
        at = block_at(block)

        def tops(t, top):
            some = acc[p, aligned(t * strip, strip, strip), at]
            return jnp.maximum(top, jnp.max(jnp.abs(some).reshape(strip // 8, 8, panel), axis=0))

        top = lax.fori_loop(0, panel // strip, tops, jnp.zeros((8, panel), F32))
        return jnp.max(top, axis=0, keepdims=True)

    def level_of(top):
        return jnp.ceil(jnp.log2(jnp.maximum(top, 1e-30)) * FINE)

    def rows_of(i):
        if i == 0:
            return pl.ds(0, 16 + counts[0])
        return pl.ds(16 + offsets[i], counts[i])

    def bound_of(source):
        return jnp.exp2(source[pl.ds(0, 16), :].astype(F32)[:1] * (1.0 / FINE))

    def quantize(p, block, i, level, target):
        at = block_at(block)
        scale = TOP * jnp.exp2(level * (-1.0 / FINE))

        @pl.loop(0, counts[i] // strip)
        def _(t):
            some = acc[p, aligned(order[i] + t * strip, strip, strip), at]
            target[aligned(16 + offsets[i] + t * strip, strip, 16), :] = (
                jnp.round(some * scale).astype(jnp.int32).astype(jnp.int16)
            )

        if i == 0:
            target[pl.ds(0, 16), :] = jnp.broadcast_to(
                level.astype(jnp.int32), (16, panel)
            ).astype(jnp.int16)

    def add_in(source, bound, block, i):
        at = block_at(block)
        scale = bound * (1.0 / TOP)

        @pl.loop(0, counts[i] // strip)
        def _(t):
            here = aligned(order[i] + t * strip, strip, strip)
            some = source[aligned(16 + offsets[i] + t * strip, strip, 16), :].astype(F32)
            acc[0, here, at] = acc[0, here, at] + some * scale

    for q in range(parts):
        held[0, held_rows(z, q), :] = m_ref[z, given_rows(q), :]
    whole[metric_rows, :] = metric_pad[...]

    @pl.when(end)
    def _():
        for r, q in (
            (FAR_END, 0), (FAR_END, 1), (FAR_END, 2), (FAR_END, 3), (FAR_END, 4),
            (FAR_INNER, 0), (FAR_INNER, 1), (MATE, 0), (MATE, 1),
        ):
            arrive(r, q)

    @pl.when(jnp.logical_not(end))
    def _():
        for r, q in (
            (MATE, 0), (MATE, 1), (FAR_END, 0), (FAR_END, 1), (MATE, 2), (FAR_INNER, 0),
            (MATE, 3), (FAR_INNER, 1), (MATE, 4),
        ):
            arrive(r, q)

    for copy in gather:
        copy.wait_recv()
    build_kron(kron_four)
    build_kron(kron_two)
    slots_of(0)
    fit_part(0)
    turn(0, 0)
    turn(1, 0)
    contract_all(1, 0, True)
    contract_all(0, 0, True)

    @pl.when(end)
    def _():
        for q in (2, 3, 4):
            arrive(MATE, q)

    @pl.when(jnp.logical_not(end))
    def _():
        for q in (2, 3, 4):
            arrive(FAR_END, q)

    slots_of(1)
    fit_part(1)
    turn(1, 1)
    turn(0, 1)
    contract_all(1, 1, False)
    contract_all(0, 1, False)
    arrive(FAR_INNER, 2)
    arrive(FAR_INNER, 3)
    slots_of(2)
    fit_part(2)
    turn(1, 2)
    turn(0, 2)
    contract(1, 0, 2, False)
    contract(1, step, 2, False)
    arrive(FAR_INNER, 4)
    contract(1, 2 * step, 2, False)
    contract(0, far_edge, 2, False)
    slots_of(3)
    fit_part(3)
    turn(1, 3)
    contract_all(1, 3, False)
    slots_of(4)
    fit_part(4)
    turn(1, 4)

    def given(k, i):
        at, n = rows_of(i), k * pieces + i
        return remote(rs_out.at[k, at], rs_in.at[k, at], rs.at[n], rr.at[n], z, rs_peer)

    def give(k, level, i):
        quantize(1, (far, near)[k], i, level, rs_out.at[k])
        given(k, i).start()

    contract(1, far_edge, 4, False)
    contract(1, step, 4, False)
    far_level = level_of(tops_of(1, far))
    F, N = FAR, NEAR
    hold = jnp.logical_and(holder, jnp.logical_not(end))
    in_order = tuple((k, i) for k in (F, N) for i in range(pieces))
    mixed_order = (
        (F, 0), (F, 1), (F, 2), (N, 0), (F, 3), (N, 1), (F, 4), (N, 2), (F, 5), (N, 3), (N, 4), (N, 5),
    )
    hold_order = (
        (F, 0), (F, 1), (N, 0), (N, 1), (N, 2), (F, 2), (N, 3), (F, 3), (F, 4), (F, 5), (N, 4), (N, 5),
    )
    for i in range(2):
        give(FAR, far_level, i)

    @pl.when(mixed)
    def _():
        give(FAR, far_level, 2)

    @pl.when(end)
    def _():
        for i in range(2, pieces):
            give(FAR, far_level, i)

    for q in range(3, parts):
        turn(0, q)
    contract(0, far_edge, None, 3)
    contract(0, step, None, 2)
    far_top = tops_of(0, far)

    def along(k, i, into, there):
        at, n = rows_of(i), k * pieces + i
        return remote(
            rs_out.at[k, at], z_in.at[into, at], cs.at[n], cr.at[into * pieces + i], there, orb
        )

    def inward(i):
        return along(FAR, i, FAR, mate)

    def to_mate(i):
        return along(NEAR, i, NEAR, mate)

    def across(i):
        return along(FAR, i, MORE, far_inner)

    def near_given(i):
        given(NEAR, i).wait()
        add_in(rs_in.at[NEAR], bound_of(rs_in.at[NEAR]), near, i)

    def far_given(i):
        given(FAR, i).wait()
        add_in(rs_in.at[FAR], bound_of(rs_in.at[FAR]), far, i)

    def far_to_mate(i):
        far_given(i)
        quantize(0, far, i, level_of(far_top + bound_of(rs_in.at[FAR])), rs_out.at[FAR])
        inward(i).start()

    def far_across(i):
        far_given(i)
        inward(i).wait_recv()
        more = bound_of(z_in.at[FAR])
        add_in(z_in.at[FAR], more, far, i)
        total = far_top + bound_of(rs_in.at[FAR]) + more
        quantize(0, far, i, level_of(total), rs_out.at[FAR])
        across(i).start()

    own_at = block_at(near)

    def last(i):
        return remote(
            acc.at[0, aligned(order[i], counts[i], counts[i]), own_at],
            out_ref.at[pl.ds(starts[i], counts[i])], ws.at[i], wr.at[i], z, partner,
        )

    def settle(i):
        return pltpu.make_async_copy(
            acc.at[0, aligned(order[i], counts[i], counts[i]), own_at],
            out_ref.at[pl.ds(starts[i], counts[i])], ws.at[i],
        )

    @pl.when(end)
    def _():
        far_to_mate(0)

    @pl.when(jnp.logical_not(end))
    def _():
        far_across(0)

    contract(1, near_edge, 4, False)
    near_level = level_of(tops_of(1, near))
    def give_rest(sequence):
        for k, i in sequence:
            give(k, (far_level, near_level)[k], i)

    @pl.when(mixed)
    def _():
        give_rest(mixed_order[3:])

    @pl.when(hold)
    def _():
        give_rest(hold_order[2:])

    @pl.when(end)
    def _():
        give_rest(in_order[pieces:])

    contract(0, near_edge, None, 2)
    near_top = tops_of(0, near)

    def near_pass(i, combined):
        near_given(i)
        total = near_top + bound_of(rs_in.at[NEAR])
        if combined:
            across(i).wait_recv()
            more = bound_of(z_in.at[MORE])
            add_in(z_in.at[MORE], more, near, i)
            total = total + more
        quantize(0, near, i, level_of(total), rs_out.at[NEAR])
        to_mate(i).start()

    @pl.when(mixed)
    def _():
        for k, i in mixed_order[1:]:
            if k == F:
                far_across(i)
            else:
                near_pass(i, True)

    @pl.when(end)
    def _():
        for i in range(1, pieces):
            far_to_mate(i)

    @pl.when(hold)
    def _():
        for k, i in hold_order[1:]:
            if k == F:
                far_across(i)
            else:
                near_given(i)

    @pl.when(jnp.logical_and(end, jnp.logical_not(holder)))
    def _():
        for i in range(pieces):
            near_pass(i, False)

    for copy in gather:
        copy.wait_send()
    for r in range(4):
        for q in range(parts):
            if r:
                spread(r, q).wait_send()
            for copy in shares(r, q):
                copy.wait_send()

    def finish(crossed):
        for i in range(pieces):
            to_mate(i).wait_recv()
            add_in(z_in.at[NEAR], bound_of(z_in.at[NEAR]), near, i)
            if crossed:
                across(i).wait_recv()
                add_in(z_in.at[MORE], bound_of(z_in.at[MORE]), near, i)
            if i < half:
                last(i).start()
            else:
                settle(i).start()
        for i in range(half):
            last(i).wait_send()
            settle(half + i).wait()

    @pl.when(jnp.logical_and(holder, end))
    def _():
        for i in range(pieces):
            near_given(i)
        finish(False)

    @pl.when(hold)
    def _():
        finish(True)

    @pl.when(jnp.logical_not(holder))
    def _():
        for i in range(half):
            last(i).wait_recv()

    for i in range(pieces):
        inward(i).wait_send()

    @pl.when(jnp.logical_not(holder))
    def _():
        for i in range(pieces):
            to_mate(i).wait_send()


def direct(half, metric, survive):
    aux_local, occ_local, ao = half.shape
    n_aux, n_orb = lax.axis_size("aux"), lax.axis_size("orb")
    part = occ_local // n_aux
    if survive.shape[:2] != (1, 2) or part % 6:
        return plain(half, metric, survive)
    survive = survive.reshape(survive.shape[1:])
    n_fit = n_aux * aux_local
    width = -(-n_fit // 128) * 128
    sizes = (part // 3,) + (part // 6,) * 4
    parts = len(sizes)
    four, two = sizes[0] * n_fit, sizes[1] * n_fit
    late = 12 * two
    rows, panel = ao // n_orb, ao // n_aux
    dma = pltpu.SemaphoreType.DMA
    bf16, i16 = jnp.bfloat16, jnp.int16
    block = (panel + 16, panel)
    return pl.pallas_call(
        functools.partial(kernel, sizes),
        out_shape=jax.ShapeDtypeStruct((rows, panel), F32),
        in_specs=[pl.BlockSpec(memory_space=pl.ANY)] + [pl.BlockSpec(memory_space=pltpu.VMEM)] * 2,
        out_specs=pl.BlockSpec(memory_space=pl.ANY),
        scratch_shapes=[
            pltpu.VMEM((aux_local, occ_local, ao), bf16),
            pltpu.VMEM((n_aux, part * aux_local, ao), bf16),
            pltpu.VMEM((aux_local * occ_local, aux_local * occ_local), bf16),
            pltpu.VMEM((survive.shape[0], ao), F32),
            pltpu.VMEM((aux_local, width), bf16),
            pltpu.VMEM((4, part * n_fit, ao), bf16),
            pltpu.VMEM((late, 3 * panel), bf16),
            pltpu.VMEM((panel, late), bf16),
            pltpu.VMEM((panel, 4 * four), bf16),
            pltpu.VMEM((2, panel, 2 * panel), F32),
            pltpu.VMEM((n_fit, width), bf16),
            pltpu.VMEM((four, four), bf16),
            pltpu.VMEM((two, two), bf16),
            pltpu.VMEM((2, *block), i16),
            pltpu.VMEM((2, *block), i16),
            pltpu.VMEM((3, *block), i16),
            dma((6,)),
            dma((4,)), dma((4,)),
            dma((4 * parts,)), dma((n_aux * parts,)),
            dma((20 * parts,)), dma((24 * parts,)),
            dma((12,)), dma((12,)),
            dma((12,)), dma((18,)),
            dma((6,)), dma((3,)),
        ],
        compiler_params=pltpu.CompilerParams(
            collective_id=0, has_side_effects=True, vmem_limit_bytes=66 * 1000 * 1000
        ),
    )(half, metric, survive)


def solution(mesh):
    square = mesh.shape["aux"] == 4 and mesh.shape["orb"] == 8
    return jax.shard_map(
        direct if square else plain,
        mesh=mesh,
        in_specs=(P("aux", "orb", None), P("aux", None), P("aux", "orb", None)),
        out_specs=P("orb", "aux"),
        check_vma=False,
    )
```

```python
import functools

import jax
import jax.numpy as jnp
from jax import lax
from jax.experimental import pallas as pl
from jax.experimental.pallas import tpu as pltpu
from jax.sharding import PartitionSpec as P

MESH = pl.DeviceIdType.MESH
F32 = jnp.float32


def gated(half, survive):
    aux_local, occ_local, ao_count = half.shape
    blocks_aux, blocks_occ, blocks_ao = survive.shape
    gate = survive.astype(jnp.bfloat16)
    shaped = half.reshape(
        blocks_aux, aux_local, blocks_occ, occ_local // blocks_occ, blocks_ao, ao_count // blocks_ao
    )
    return (shaped * gate[:, None, :, None, :, None]).reshape(aux_local, occ_local, ao_count)


def plain(half, metric, survive):
    aux_local, occ_local, ao_count = half.shape
    portion = lax.all_gather(gated(half, survive), "aux", axis=0, tiled=True)
    fit_total = jnp.dot(metric, portion.reshape(portion.shape[0], -1), preferred_element_type=F32)
    fitted = fit_total.astype(jnp.bfloat16).reshape(aux_local, occ_local, ao_count)
    group_width = ao_count // lax.axis_size("orb")
    row_start = lax.axis_index("orb") * group_width
    flat_rows = lax.all_gather(fitted, "orb", axis=1, tiled=True).reshape(-1, ao_count)
    left_rows = lax.dynamic_slice_in_dim(flat_rows, row_start, group_width, 1)
    partial_k = lax.dot_general(
        left_rows, flat_rows, (((0,), (0,)), ((), ())), preferred_element_type=F32
    )
    return lax.psum_scatter(partial_k, "aux", scatter_dimension=1, tiled=True)

TOP = 32000.0
FINE = 256.0


def kernel(
    sizes, half_ref, metric_ref, survive_ref, out_ref, raw, m_ref, pick_ref, gate, metric_pad, held, fit, left, early, acc, whole, kron_four, kron_two,
    rs_out, rs_in, z_in,
    ls, gs, gr, zs, zr, fs, fr, rs, rr, cs, cr, ws, wr,
):
    z = lax.axis_index("aux")
    orb = lax.axis_index("orb")
    n_aux = m_ref.shape[0]
    aux_local, occ_local, ao = raw.shape
    parts = len(sizes)
    begins = [sum(sizes[:q]) for q in range(parts)]
    panel = acc.shape[1]
    unit_rows = panel // 8
    counts = [n * unit_rows for n in (1, 1, 2, 2, 1, 1)]
    starts = [n * unit_rows for n in (0, 1, 2, 0, 2, 3)]
    offsets = [n * unit_rows for n in (0, 1, 2, 4, 6, 7)]
    pieces = len(counts)
    chip = orb // 2
    core = orb % 2
    x, y = chip % 2, chip // 2
    x_chip = chip + 1 - 2 * x
    y_chip = chip + 2 - 4 * y
    partner = orb + 1 - 2 * core
    other_chip = core * x_chip + (1 - core) * y_chip
    rs_peer = 2 * other_chip + core
    unused = core * (3 - 3 * y) + (1 - core) * (1 + x)
    odd_panel = 6 - unused - 3
    side = z // 2
    end = z % 3 == 0
    mate = z + 1 - 2 * (z % 2)
    far_end = 3 - 3 * side
    far_inner = 2 - side
    near_block = core * (1 + side) + (1 - core) * 3 * side
    far_block = 3 - near_block
    holder = near_block == z

    barrier = pltpu.get_barrier_semaphore()
    for d in (1, 2, 3):
        pl.semaphore_signal(
            barrier, inc=1, device_id={"aux": (z + d) % n_aux, "orb": orb}, device_id_type=MESH
        )
    for o in (partner, 2 * x_chip, 2 * x_chip + 1, 2 * y_chip, 2 * y_chip + 1):
        pl.semaphore_signal(barrier, inc=1, device_id={"aux": z, "orb": o}, device_id_type=MESH)

    tiles = ls.shape[0]
    tile_width = ao // tiles
    loads = []
    for t in range(tiles):
        at = pl.ds(t * tile_width, tile_width)
        load = pltpu.make_async_copy(half_ref.at[:, :, at], raw.at[:, :, at], ls.at[t])
        load.start()
        loads.append(load)

    count = aux_local * occ_local
    out_row = lax.broadcasted_iota(jnp.int32, (count, count), 0)
    in_row = lax.broadcasted_iota(jnp.int32, (count, count), 1)
    wanted = lax.rem(out_row, aux_local) * occ_local + lax.div(out_row, aux_local)
    pick_ref[...] = jnp.where(in_row == wanted, 1.0, 0.0).astype(pick_ref.dtype)
    survived = survive_ref[...].astype(F32)
    ao_blocks = survive_ref.shape[1]
    block_width = ao // ao_blocks
    for b in range(ao_blocks):
        gate[:, pl.ds(b * block_width, block_width)] = jnp.broadcast_to(
            survived[:, b : b + 1], (gate.shape[0], block_width)
        )
    metric_pad[...] = jnp.zeros_like(metric_pad)
    metric_pad[:, pl.ds(0, metric_ref.shape[1])] = metric_ref[...]

    def remote(src, dst, send, recv, a, o):
        return pltpu.make_async_remote_copy(
            src_ref=src, dst_ref=dst, send_sem=send, recv_sem=recv,
            device_id={"aux": a, "orb": o}, device_id_type=MESH,
        )

    def aligned(start, size, unit_of=128):
        return pl.ds(pl.multiple_of(start, unit_of), size)

    def given_rows(q):
        return pl.ds(begins[q] * aux_local, sizes[q] * aux_local)

    def held_rows(source, q):
        unit = sizes[q] * aux_local
        return aligned(begins[q] * aux_local * n_aux + source * unit, unit, unit)

    MATE, FAR_END, FAR_INNER = 1, 2, 3
    sources = (z, mate, far_end, far_inner)

    def spread(r, q):
        there = sources[r]
        return remote(
            m_ref.at[there, given_rows(q)], held.at[0, held_rows(z, q)],
            zs.at[r * parts + q], zr.at[z * parts + q], there, orb,
        )

    def sort_rows(dest, dests, first):
        span = dests * count // n_aux
        rows_at = pl.multiple_of(dest * (count // n_aux), count // n_aux)
        pair = dest // 2
        for t in range(tiles):
            at = pl.ds(t * tile_width, tile_width)
            if first:
                loads[t].wait()
            sorted_rows = jnp.dot(
                pick_ref[pl.ds(rows_at, span), :], raw[:, :, at].reshape(count, tile_width),
                preferred_element_type=F32,
            )
            gated_rows = sorted_rows * gate[pl.ds(pair, 1), at]
            m_ref[pl.ds(dest, dests), :, at] = gated_rows.astype(m_ref.dtype).reshape(
                dests, count // n_aux, tile_width
            )

    sort_rows(far_end, 1, True)
    pl.semaphore_wait(barrier, 8)

    metric_rows = aligned(z * aux_local, aux_local, aux_local)
    gather = []
    for d in (1, 3, 2):
        copy = remote(metric_pad, whole.at[metric_rows], gs.at[d], gr.at[d], (z + d) % n_aux, orb)
        copy.start()
        gather.append(copy)

    @pl.when(end)
    def _():
        for q in range(parts):
            spread(FAR_END, q).start()

    @pl.when(jnp.logical_not(end))
    def _():
        for q in range(2):
            spread(FAR_END, q).start()

    sort_rows(far_inner, 1, False)

    @pl.when(jnp.logical_not(end))
    def _():
        for r, q in (
            (FAR_INNER, 0), (FAR_INNER, 1), (FAR_END, 2), (FAR_END, 3), (FAR_END, 4),
            (FAR_INNER, 2), (FAR_INNER, 3), (FAR_INNER, 4),
        ):
            spread(r, q).start()

    sort_rows(2 * side, 2, False)

    @pl.when(end)
    def _():
        for r, q in (
            (MATE, 0), (MATE, 1), (FAR_INNER, 0), (FAR_INNER, 1), (MATE, 2),
            (MATE, 3), (MATE, 4), (FAR_INNER, 2), (FAR_INNER, 3), (FAR_INNER, 4),
        ):
            spread(r, q).start()

    @pl.when(jnp.logical_not(end))
    def _():
        for q in range(parts):
            spread(MATE, q).start()

    def recv_at(slot, r, q, k):
        return fr.at[(((slot - 1) * 4 + r) * parts + q) * 2 + k]

    def shares(r, q):
        source = sources[r]
        at = held_rows(source, q)

        def cut(columns):
            if r == 0:
                return m_ref.at[z, given_rows(q), columns]
            return held.at[0, at, columns]

        jobs = [(partner, 1, pl.ds(0, 4 * panel), 0)]
        for o, slot, first, pair in (
            (2 * x_chip, 2 + core, 3 - 3 * x, 2 * x),
            (2 * y_chip + 1, 2 + core, 1 - y, 2 - y),
        ):
            jobs += [
                (o, slot, aligned(first * panel, panel), 0),
                (o, slot, aligned(pair * panel, 2 * panel), 1),
            ]
        return [
            remote(
                cut(columns), held.at[slot, at, columns],
                fs.at[(n * 4 + r) * parts + q], recv_at(slot, r, q, k), z, o,
            )
            for n, (o, slot, columns, k) in enumerate(jobs)
        ]

    def share(r, q):
        for copy in shares(r, q):
            copy.start()

    def arrive(r, q):
        here = held.at[0, held_rows(sources[r], q)]
        remote(here, here, zs.at[q], zr.at[sources[r] * parts + q], mate, orb).wait_recv()
        share(r, q)

    for q in range(parts):
        share(0, q)

    def slots_of(q):
        first = core * y + (1 - core) * 3 * x
        pair = core * (1 + y) + (1 - core) * 2 * (1 - x)
        one, two = aligned(first * panel, panel), aligned(pair * panel, 2 * panel)
        for r in range(4):
            at = held_rows(sources[r], q)
            for slot, k, columns in (
                (1, 0, pl.ds(0, 4 * panel)), (2, 0, one), (2, 1, two), (3, 0, one), (3, 1, two)
            ):
                here = held.at[slot, at, columns]
                remote(here, here, fs.at[0], recv_at(slot, r, q, k), z, partner).wait_recv()

    def build_kron(kron_ref):
        depth, wide = kron_ref.shape[0], whole.shape[1]
        unit = depth // n_aux

        def aux_of(r):
            return lax.div(r, unit) * aux_local + lax.rem(r, aux_local)

        def orbital_of(r):
            return lax.div(lax.rem(r, unit), aux_local)

        i32, bf16 = jnp.int32, kron_ref.dtype
        by_row = aux_of(lax.broadcasted_iota(i32, (wide, depth), 1))
        pick = jnp.where(by_row == lax.broadcasted_iota(i32, (wide, depth), 0), 1.0, 0.0)
        spread_cols = jnp.dot(whole[...], pick.astype(bf16), preferred_element_type=F32).astype(bf16)
        by_col = aux_of(lax.broadcasted_iota(i32, (depth, whole.shape[0]), 0))
        take = jnp.where(by_col == lax.broadcasted_iota(i32, (depth, whole.shape[0]), 1), 1.0, 0.0)
        both = jnp.dot(take.astype(bf16), spread_cols, preferred_element_type=F32)
        same = orbital_of(lax.broadcasted_iota(i32, (depth, depth), 0)) == orbital_of(
            lax.broadcasted_iota(i32, (depth, depth), 1)
        )
        kron_ref[...] = jnp.where(same, both, 0.0).astype(bf16)

    def place(p):
        return jnp.where(p == core, 0, jnp.where(p == 3 - core, 1, 2))

    def depth_of(q):
        return 4 * sizes[q] * aux_local * n_aux

    fit_at = (0, 0, 0, depth_of(2), 2 * depth_of(2))

    def fit_part(q):
        slab = sizes[q] * aux_local * n_aux
        kron_ref = kron_four if sizes[q] == sizes[0] else kron_two
        base = begins[q] * aux_local * n_aux

        @pl.loop(0, 4)
        def _(slot):
            for n, p in enumerate((core, 3 - core, odd_panel)):
                fit[aligned(fit_at[q] + slot * slab, slab, slab), pl.ds(n * panel, panel)] = jnp.dot(
                    kron_ref[...], held[slot, pl.ds(base, slab), aligned(p * panel, panel)],
                    preferred_element_type=F32,
                ).astype(fit.dtype)

    def turn(p, q):
        chosen = other_chip if p else chip
        fitted = fit[pl.ds(fit_at[q], depth_of(q)), aligned(place(chosen) * panel, panel)]
        if p:
            early[:, pl.ds(0, depth_of(q))] = fitted.T
        else:
            left[:, pl.ds(fit_at[q], depth_of(q))] = fitted.T

    step = 2 * panel // 3
    mixed = jnp.logical_not(jnp.logical_or(end, holder))
    far_edge, near_edge = (1 - side) * 2 * step, side * 2 * step

    def contract(p, tile, q, begin):
        at = aligned(tile, step)
        if q is None:
            late = pl.ds(fit_at[begin], fit_at[-1] + depth_of(parts - 1) - fit_at[begin])
            more = jnp.dot(left[:, late], fit[late, at], preferred_element_type=F32)
        elif p:
            more = jnp.dot(
                early[:, pl.ds(0, depth_of(q))], fit[pl.ds(fit_at[q], depth_of(q)), at],
                preferred_element_type=F32,
            )
        else:
            more = jnp.dot(
                left[:, pl.ds(fit_at[q], depth_of(q))], fit[pl.ds(fit_at[q], depth_of(q)), at],
                preferred_element_type=F32,
            )
        acc[p, :, at] = more if begin is True else acc[p, :, at] + more

    def contract_all(p, q, begin):
        @pl.loop(0, 3)
        def _(t):
            contract(p, t * step, q, begin)

    near, far = side, 1 - side
    strip = 32
    half = pieces // 2
    sides_of = [1 - core] * half + [core] * half
    order = [sides_of[i] * 4 * unit_rows + starts[i] for i in range(pieces)]
    FAR, NEAR, MORE = 0, 1, 2

    def block_at(block):
        return aligned(block * panel, panel)

    def tops_of(p, block):
        at = block_at(block)

        def tops(t, top):
            some = acc[p, aligned(t * strip, strip, strip), at]
            return jnp.maximum(top, jnp.max(jnp.abs(some).reshape(strip // 8, 8, panel), axis=0))

        top = lax.fori_loop(0, panel // strip, tops, jnp.zeros((8, panel), F32))
        return jnp.max(top, axis=0, keepdims=True)

    def level_of(top):
        return jnp.ceil(jnp.log2(jnp.maximum(top, 1e-30)) * FINE)

    def rows_of(i):
        if i == 0:
            return pl.ds(0, 16 + counts[0])
        return pl.ds(16 + offsets[i], counts[i])

    def bound_of(source):
        return jnp.exp2(source[pl.ds(0, 16), :].astype(F32)[:1] * (1.0 / FINE))

    def quantize(p, block, i, level, target):
        at = block_at(block)
        scale = TOP * jnp.exp2(level * (-1.0 / FINE))

        @pl.loop(0, counts[i] // strip)
        def _(t):
            some = acc[p, aligned(order[i] + t * strip, strip, strip), at]
            target[aligned(16 + offsets[i] + t * strip, strip, 16), :] = (
                jnp.round(some * scale).astype(jnp.int32).astype(jnp.int16)
            )

        if i == 0:
            target[pl.ds(0, 16), :] = jnp.broadcast_to(
                level.astype(jnp.int32), (16, panel)
            ).astype(jnp.int16)

    def add_in(source, bound, block, i):
        at = block_at(block)
        scale = bound * (1.0 / TOP)

        @pl.loop(0, counts[i] // strip)
        def _(t):
            here = aligned(order[i] + t * strip, strip, strip)
            some = source[aligned(16 + offsets[i] + t * strip, strip, 16), :].astype(F32)
            acc[0, here, at] = acc[0, here, at] + some * scale

    for q in range(parts):
        held[0, held_rows(z, q), :] = m_ref[z, given_rows(q), :]
    whole[metric_rows, :] = metric_pad[...]

    @pl.when(end)
    def _():
        for r, q in (
            (FAR_END, 0), (FAR_END, 1), (FAR_END, 2), (FAR_END, 3), (FAR_END, 4),
            (FAR_INNER, 0), (FAR_INNER, 1), (MATE, 0), (MATE, 1),
        ):
            arrive(r, q)

    @pl.when(jnp.logical_not(end))
    def _():
        for r, q in (
            (MATE, 0), (MATE, 1), (FAR_END, 0), (FAR_END, 1), (MATE, 2), (FAR_INNER, 0),
            (MATE, 3), (FAR_INNER, 1), (MATE, 4),
        ):
            arrive(r, q)

    for copy in gather:
        copy.wait_recv()
    build_kron(kron_four)
    build_kron(kron_two)
    slots_of(0)
    fit_part(0)
    turn(0, 0)
    turn(1, 0)
    contract_all(1, 0, True)
    contract_all(0, 0, True)

    @pl.when(end)
    def _():
        for q in (2, 3, 4):
            arrive(MATE, q)

    @pl.when(jnp.logical_not(end))
    def _():
        for q in (2, 3, 4):
            arrive(FAR_END, q)

    slots_of(1)
    fit_part(1)
    turn(1, 1)
    turn(0, 1)
    contract_all(1, 1, False)
    contract_all(0, 1, False)
    arrive(FAR_INNER, 2)
    arrive(FAR_INNER, 3)
    slots_of(2)
    fit_part(2)
    turn(1, 2)
    turn(0, 2)
    contract(1, 0, 2, False)
    contract(1, step, 2, False)
    arrive(FAR_INNER, 4)
    contract(1, 2 * step, 2, False)
    contract(0, far_edge, 2, False)
    slots_of(3)
    fit_part(3)
    turn(1, 3)
    contract_all(1, 3, False)
    slots_of(4)
    fit_part(4)
    turn(1, 4)

    def given(k, i):
        at, n = rows_of(i), k * pieces + i
        return remote(rs_out.at[k, at], rs_in.at[k, at], rs.at[n], rr.at[n], z, rs_peer)

    def give(k, level, i):
        quantize(1, (far, near)[k], i, level, rs_out.at[k])
        given(k, i).start()

    contract(1, far_edge, 4, False)
    contract(1, step, 4, False)
    far_level = level_of(tops_of(1, far))
    F, N = FAR, NEAR
    hold = jnp.logical_and(holder, jnp.logical_not(end))
    in_order = tuple((k, i) for k in (F, N) for i in range(pieces))
    mixed_order = (
        (F, 0), (F, 1), (F, 2), (N, 0), (F, 3), (N, 1), (F, 4), (N, 2), (F, 5), (N, 3), (N, 4), (N, 5),
    )
    hold_order = (
        (F, 0), (F, 1), (N, 0), (N, 1), (N, 2), (F, 2), (N, 3), (F, 3), (F, 4), (F, 5), (N, 4), (N, 5),
    )
    for i in range(2):
        give(FAR, far_level, i)

    @pl.when(mixed)
    def _():
        give(FAR, far_level, 2)

    @pl.when(end)
    def _():
        for i in range(2, pieces):
            give(FAR, far_level, i)

    for q in range(3, parts):
        turn(0, q)
    contract(0, far_edge, None, 3)
    contract(0, step, None, 2)
    far_top = tops_of(0, far)

    def along(k, i, into, there):
        at, n = rows_of(i), k * pieces + i
        return remote(
            rs_out.at[k, at], z_in.at[into, at], cs.at[n], cr.at[into * pieces + i], there, orb
        )

    def inward(i):
        return along(FAR, i, FAR, mate)

    def to_mate(i):
        return along(NEAR, i, NEAR, mate)

    def across(i):
        return along(FAR, i, MORE, far_inner)

    def near_given(i):
        given(NEAR, i).wait()
        add_in(rs_in.at[NEAR], bound_of(rs_in.at[NEAR]), near, i)

    def far_given(i):
        given(FAR, i).wait()
        add_in(rs_in.at[FAR], bound_of(rs_in.at[FAR]), far, i)

    def far_to_mate(i):
        far_given(i)
        quantize(0, far, i, level_of(far_top + bound_of(rs_in.at[FAR])), rs_out.at[FAR])
        inward(i).start()

    def far_across(i):
        far_given(i)
        inward(i).wait_recv()
        more = bound_of(z_in.at[FAR])
        add_in(z_in.at[FAR], more, far, i)
        total = far_top + bound_of(rs_in.at[FAR]) + more
        quantize(0, far, i, level_of(total), rs_out.at[FAR])
        across(i).start()

    own_at = block_at(near)

    def last(i):
        return remote(
            acc.at[0, aligned(order[i], counts[i], counts[i]), own_at],
            out_ref.at[pl.ds(starts[i], counts[i])], ws.at[i], wr.at[i], z, partner,
        )

    def settle(i):
        return pltpu.make_async_copy(
            acc.at[0, aligned(order[i], counts[i], counts[i]), own_at],
            out_ref.at[pl.ds(starts[i], counts[i])], ws.at[i],
        )

    @pl.when(end)
    def _():
        far_to_mate(0)

    @pl.when(jnp.logical_not(end))
    def _():
        far_across(0)

    contract(1, near_edge, 4, False)
    near_level = level_of(tops_of(1, near))
    def give_rest(sequence):
        for k, i in sequence:
            give(k, (far_level, near_level)[k], i)

    @pl.when(mixed)
    def _():
        give_rest(mixed_order[3:])

    @pl.when(hold)
    def _():
        give_rest(hold_order[2:])

    @pl.when(end)
    def _():
        give_rest(in_order[pieces:])

    contract(0, near_edge, None, 2)
    near_top = tops_of(0, near)

    def near_pass(i, combined):
        near_given(i)
        total = near_top + bound_of(rs_in.at[NEAR])
        if combined:
            across(i).wait_recv()
            more = bound_of(z_in.at[MORE])
            add_in(z_in.at[MORE], more, near, i)
            total = total + more
        quantize(0, near, i, level_of(total), rs_out.at[NEAR])
        to_mate(i).start()

    @pl.when(mixed)
    def _():
        for k, i in mixed_order[1:]:
            if k == F:
                far_across(i)
            else:
                near_pass(i, True)

    @pl.when(end)
    def _():
        for i in range(1, pieces):
            far_to_mate(i)

    @pl.when(hold)
    def _():
        for k, i in hold_order[1:]:
            if k == F:
                far_across(i)
            else:
                near_given(i)

    @pl.when(jnp.logical_and(end, jnp.logical_not(holder)))
    def _():
        for i in range(pieces):
            near_pass(i, False)

    for copy in gather:
        copy.wait_send()
    for r in range(4):
        for q in range(parts):
            if r:
                spread(r, q).wait_send()
            for copy in shares(r, q):
                copy.wait_send()

    def finish(crossed):
        for i in range(pieces):
            to_mate(i).wait_recv()
            add_in(z_in.at[NEAR], bound_of(z_in.at[NEAR]), near, i)
            if crossed:
                across(i).wait_recv()
                add_in(z_in.at[MORE], bound_of(z_in.at[MORE]), near, i)
            if i < half:
                last(i).start()
            else:
                settle(i).start()
        for i in range(half):
            last(i).wait_send()
            settle(half + i).wait()

    @pl.when(jnp.logical_and(holder, end))
    def _():
        for i in range(pieces):
            near_given(i)
        finish(False)

    @pl.when(hold)
    def _():
        finish(True)

    @pl.when(jnp.logical_not(holder))
    def _():
        for i in range(half):
            last(i).wait_recv()

    for i in range(pieces):
        inward(i).wait_send()

    @pl.when(jnp.logical_not(holder))
    def _():
        for i in range(pieces):
            to_mate(i).wait_send()


def direct(half, metric, survive):
    aux_local, occ_local, ao = half.shape
    n_aux, n_orb = lax.axis_size("aux"), lax.axis_size("orb")
    part = occ_local // n_aux
    if survive.shape[:2] != (1, 2) or part % 6:
        return plain(half, metric, survive)
    survive = survive.reshape(survive.shape[1:])
    n_fit = n_aux * aux_local
    width = -(-n_fit // 128) * 128
    sizes = (part // 3,) + (part // 6,) * 4
    parts = len(sizes)
    four, two = sizes[0] * n_fit, sizes[1] * n_fit
    late = 12 * two
    rows, panel = ao // n_orb, ao // n_aux
    dma = pltpu.SemaphoreType.DMA
    bf16, i16 = jnp.bfloat16, jnp.int16
    block = (panel + 16, panel)
    return pl.pallas_call(
        functools.partial(kernel, sizes),
        out_shape=jax.ShapeDtypeStruct((rows, panel), F32),
        in_specs=[pl.BlockSpec(memory_space=pl.ANY)] + [pl.BlockSpec(memory_space=pltpu.VMEM)] * 2,
        out_specs=pl.BlockSpec(memory_space=pl.ANY),
        scratch_shapes=[
            pltpu.VMEM((aux_local, occ_local, ao), bf16),
            pltpu.VMEM((n_aux, part * aux_local, ao), bf16),
            pltpu.VMEM((aux_local * occ_local, aux_local * occ_local), bf16),
            pltpu.VMEM((survive.shape[0], ao), F32),
            pltpu.VMEM((aux_local, width), bf16),
            pltpu.VMEM((4, part * n_fit, ao), bf16),
            pltpu.VMEM((late, 3 * panel), bf16),
            pltpu.VMEM((panel, late), bf16),
            pltpu.VMEM((panel, 4 * four), bf16),
            pltpu.VMEM((2, panel, 2 * panel), F32),
            pltpu.VMEM((n_fit, width), bf16),
            pltpu.VMEM((four, four), bf16),
            pltpu.VMEM((two, two), bf16),
            pltpu.VMEM((2, *block), i16),
            pltpu.VMEM((2, *block), i16),
            pltpu.VMEM((3, *block), i16),
            dma((6,)),
            dma((4,)), dma((4,)),
            dma((4 * parts,)), dma((n_aux * parts,)),
            dma((20 * parts,)), dma((24 * parts,)),
            dma((12,)), dma((12,)),
            dma((12,)), dma((18,)),
            dma((6,)), dma((3,)),
        ],
        compiler_params=pltpu.CompilerParams(
            collective_id=0, has_side_effects=True, vmem_limit_bytes=66 * 1000 * 1000
        ),
    )(half, metric, survive)


def solution(mesh):
    square = mesh.shape["aux"] == 4 and mesh.shape["orb"] == 8
    return jax.shard_map(
        direct if square else plain,
        mesh=mesh,
        in_specs=(P("aux", "orb", None), P("aux", None), P("aux", "orb", None)),
        out_specs=P("orb", "aux"),
        check_vma=False,
    )
```
